128 devices in a mesh: row: 64 (over z, y, x), col: 2 (over core).
Axes of the slice: x: 4, y: 4, z: 4, core: 2. Of those that a mesh axis runs over, the one named last changes fastest.
Arguments:
- pencil_left: bfloat16 [1, 64, 256, 4, 2, 256], P(None, 'row', None, None, 'col'), may hold values from -0.09375 to 0.09375
- pencil_right: bfloat16 [1, 64, 256, 4, 2, 256], P(None, 'row', None, None, 'col'), may hold values from -0.09375 to 0.09375
- basis_panel: bfloat16 [1, 64, 256, 4, 2, 256], P(None, 'row', None, None, 'col'), may hold values from -0.125 to 0.125
- block_inverses: float32 [4, 2, 256, 256], replicated, may hold values from -0.2 to 2.3
- pencil_shift: float32 [], replicated, may hold values from 0.5 to 1.5
- start_vectors: float32 [1, 64, 256, 512], P(None, 'row', None, 'col'), may hold values from -6 to 6
Outputs:
- pending: float32 [1, 64, 256, 512], P(None, 'row', None, 'col')
- image: float32 [1, 64, 256, 512], P(None, 'row', None, 'col')
The draws below stay inside these ranges and needn't reach their ends.
All inputs are finite; a program needn't handle non-finite values.
Results may differ from the reference program's by a relative error of at most 0.0043.
Values may be sent and summed in bfloat16 or wider, within the bound.
No kernel may reach another device: no remote copies, remote signals or barrier semaphores. Data moves between devices by JAX's collectives and lax.ppermute only.
A program may use at most 64 MiB of HBM per device.

```python
import math
import jax
import jax.numpy as jnp
from jax import lax

ORDER = 16384
NB = 256
STEPS = 8
NEV = 512
RB = 1
PB = 4
N_ROW = 64
N_COL = 2


def draw_block_inverses(key, part):
    first_key, second_key = jax.random.split(jax.random.fold_in(key, 17))
    scales = jnp.exp(jax.random.uniform(first_key, (PB, N_COL, NB), jnp.float32, -0.7, 0.7))
    spread = jnp.clip(jax.random.normal(second_key, (PB, N_COL, NB, NB), jnp.float32), -5.0, 5.0)
    spread = jnp.clip(spread * (0.6 / math.sqrt(NB)), -0.19, 0.19)
    identity = jnp.eye(NB, dtype=jnp.float32)
    return identity * scales[..., None] + spread


def steps_of(own_key, dims, shards, low, top_value):
    factor_of = 1.0
    for position, parts in shards:
        draws = jax.random.uniform(jax.random.fold_in(jax.random.fold_in(own_key, 6), position), (parts,), jnp.float32, low / len(shards), top_value / len(shards))
        factor_of = factor_of * jnp.repeat(jnp.exp(draws), dims[position] // parts).reshape((-1,) + (1,) * (len(dims) - 1 - position))
    return factor_of


def normal_values(rng, shape, width, most, pieces=(), kind=jnp.bfloat16):
    level = steps_of(rng, shape, pieces, -0.22, 0.18) if pieces else 1.0
    array = jax.random.normal(rng, shape, jnp.float32) * width * level
    return jnp.minimum(jnp.maximum(array, -most), most).astype(kind)


def setup_inputs(seed: int = 0) -> dict:
    key_of = jax.random.split(jax.random.key(seed), 7)
    return {
        "pencil_left": normal_values(key_of[0], (RB, N_ROW, NB, PB, N_COL, NB), (2 * STEPS * NB) ** -0.5, 0.09375, ((1, 64), (4, 2))),
        "pencil_right": normal_values(key_of[1], (RB, N_ROW, NB, PB, N_COL, NB), (2 * STEPS * NB) ** -0.5, 0.09375, ((1, 64), (4, 2))),
        "basis_panel": normal_values(key_of[2], (RB, N_ROW, NB, PB, N_COL, NB), (STEPS * NB) ** -0.5, 0.125, ((1, 64), (4, 2))),
        "block_inverses": draw_block_inverses(jax.random.fold_in(key_of[6], 71), 0),
        "pencil_shift": jnp.clip(jax.random.uniform(key_of[4], (), jnp.float32, 0.5, 1.5), 0.5, 1.5),
        "start_vectors": normal_values(key_of[5], (RB, N_ROW, NB, NEV), 1.0, 6.0, ((1, 64), (3, 2)), jnp.float32),
    }


def reference(pencil_left, pencil_right, basis_panel, block_inverses, pencil_shift, start_vectors):
    panel_width = STEPS * NB
    left_whole = pencil_left.reshape(ORDER, panel_width)
    right_whole = pencil_right.reshape(ORDER, panel_width)
    basis_whole = basis_panel.reshape(ORDER, panel_width)
    inverse_blocks = block_inverses.reshape(STEPS, NB, NB)
    pending = start_vectors.reshape(ORDER, NEV).astype(jnp.float32)
    first_block = ORDER // NB - STEPS
    row_blocks = jnp.arange(ORDER // NB, dtype=jnp.int32)
    solved = []
    for column in range(STEPS - 1, -1, -1):
        target = first_block + column
        block_rhs = pending[target * NB:(target + 1) * NB]
        vectors = jnp.dot(inverse_blocks[column], block_rhs, precision=lax.Precision.HIGHEST).astype(jnp.bfloat16)
        solved.append(vectors)
        left_cols = left_whole[:, column * NB:(column + 1) * NB]
        right_cols = right_whole[:, column * NB:(column + 1) * NB]
        update = jnp.dot(left_cols, vectors, preferred_element_type=jnp.float32) - pencil_shift * jnp.dot(right_cols, vectors, preferred_element_type=jnp.float32)
        above = (row_blocks < target)[:, None, None]
        update = jnp.where(above, update.reshape(ORDER // NB, NB, NEV), jnp.float32(0.0)).reshape(ORDER, NEV)
        pending = pending - update
    solved_all = jnp.concatenate(solved[::-1], axis=0)
    image = jnp.dot(basis_whole, solved_all, preferred_element_type=jnp.float32)
    return pending.reshape(RB, N_ROW, NB, NEV), image.reshape(RB, N_ROW, NB, NEV)
```

```python
import jax
import jax.numpy as jnp
from jax import lax
from jax.experimental import pallas as pl
from jax.experimental.pallas import tpu as pltpu
from jax.sharding import Mesh, PartitionSpec as P

STEPS = 8
HALF = STEPS // 2
NB = 256
RING = 4
SUB = 8
ROWS = ("z", "yh", "yl", "x")
GROUPS = 8
MINE = NB // RING


def times(a, b, **kw):
    return lax.dot_general(a, b, (((1,), (1,)), ((), ())), preferred_element_type=jnp.float32, **kw)


def back_substitute(where_ref, base, inv_ref, rhs, own_ref, other_ref, x_ref):
    chip, parity = where_ref[0], where_ref[1]
    x_ref[...] = jnp.zeros_like(x_ref)
    for row in range(RING - 1, -1, -1):
        acc = rhs[row]
        source = lax.rem(chip - row + RING, RING)
        for b in range(RING // 2 - 1, (row - 1) // 2, -1):
            for ref, p in ((other_ref, 1 - parity), (own_ref, parity)):
                acc = acc - times(x_ref[2 * b + p].astype(jnp.bfloat16), ref[source, b])
        x = times(acc, inv_ref[base + row], precision=lax.Precision.HIGHEST)
        x_ref[row] = x.astype(jnp.bfloat16).astype(jnp.float32)


def upper_kernel(where_ref, inv_ref, rhs_ref, own_ref, other_ref, out_ref, x_ref):
    rhs = [rhs_ref[r] for r in range(RING)]
    back_substitute(where_ref, RING, inv_ref, rhs, own_ref, other_ref, x_ref)
    for r in range(RING):
        out_ref[:, r * NB : (r + 1) * NB] = x_ref[r].astype(jnp.bfloat16)


def lower_kernel(
    where_ref, inv_ref, rhs_ref, solved_ref, far_own_ref, far_other_ref, own_ref, other_ref,
    out_ref, x_ref,
):
    chip, parity = where_ref[0], where_ref[1]
    rhs = []
    for row in range(RING):
        acc = rhs_ref[row]
        source = lax.rem(chip - row + RING, RING)
        for b in range(RING // 2):
            for ref, p in ((far_other_ref, 1 - parity), (far_own_ref, parity)):
                at = pl.multiple_of((2 * b + p) * NB, NB)
                acc = acc - times(solved_ref[:, pl.ds(at, NB)], ref[source, b])
        rhs.append(acc)
    back_substitute(where_ref, 0, inv_ref, rhs, own_ref, other_ref, x_ref)
    for r in range(RING):
        out_ref[:, r * NB : (r + 1) * NB] = x_ref[r].astype(jnp.bfloat16)


def final_kernel(
    where_ref, x_ref, w_own_ref, w_other_ref, z_own_ref, z_other_ref, rhs_ref, pending_ref, image_ref
):
    parity = where_ref[1]
    pending = rhs_ref[...]
    image = jnp.zeros_like(pending)
    for b in range(HALF):
        for w, z, p in ((w_own_ref, z_own_ref, parity), (w_other_ref, z_other_ref, 1 - parity)):
            at = pl.multiple_of((2 * (b % 2) + p) * NB, NB)
            x = x_ref[:, b // 2, :, pl.ds(at, NB)].reshape(NB, NB)
            pending = pending - times(w[b], x)
            image = image + times(z[b], x)
    pending_ref[...] = pending
    image_ref[...] = image


def call(kernel, name, outs, scratch, *args, limit=20 << 20):
    vmem = pl.BlockSpec(memory_space=pltpu.VMEM)
    return pl.pallas_call(
        kernel,
        out_shape=outs,
        in_specs=[pl.BlockSpec(memory_space=pltpu.SMEM)] + [vmem] * (len(args) - 1),
        out_specs=jax.tree.map(lambda _: vmem, outs),
        scratch_shapes=scratch,
        compiler_params=pltpu.CompilerParams(vmem_limit_bytes=limit),
        name=name,
    )(*args)


def shifted(a, step):
    return lax.ppermute(a, "x", [(i, (i + step) % RING) for i in range(RING)])


def ring_gather(a):
    return jnp.stack([a] + [shifted(a, s) for s in range(1, RING)])


def swapped(a):
    return lax.ppermute(a, "col", [(0, 1), (1, 0)])


def local(pencil_left, pencil_right, basis_panel, block_inverses, pencil_shift, start_vectors):
    row = lax.axis_index(ROWS)
    chip = lax.axis_index("x")
    parity = lax.axis_index("col")
    where = jnp.stack([chip, parity]).astype(jnp.int32)
    first = lax.axis_size(ROWS) - STEPS

    left = pencil_left.reshape(NB, HALF, NB)
    right = pencil_right.reshape(NB, HALF, NB)
    own_z = jnp.transpose(basis_panel.reshape(NB, HALF, NB), (1, 0, 2))
    rhs = start_vectors.reshape(NB, NB)
    inverses = block_inverses.reshape(STEPS, NB, NB)

    cols = 2 * jnp.arange(HALF) + parity
    live = (row < first + cols)[None, :, None]
    both = left.astype(jnp.float32) - pencil_shift * right.astype(jnp.float32)
    own_w = jnp.transpose(jnp.where(live, both, 0.0).astype(jnp.bfloat16), (1, 0, 2))

    far_own = ring_gather(own_w[HALF // 2 :])
    flipped = rhs.T.reshape(GROUPS, RING, SUB, NB).transpose(1, 0, 2, 3).reshape(RING, MINE, NB)
    ring_rhs = lax.all_to_all(flipped, "x", 0, 0, tiled=True)
    near_own = ring_gather(own_w[: HALF // 2])
    far_other = swapped(far_own)
    near_other = swapped(near_own)
    other_w = swapped(own_w)
    other_z = swapped(own_z)

    solved_shape = jax.ShapeDtypeStruct((MINE, RING * NB), jnp.bfloat16)
    scratch = [pltpu.VMEM((RING, MINE, NB), jnp.float32)]
    upper = call(
        upper_kernel, "upper", solved_shape, scratch,
        where, inverses, ring_rhs, far_own, far_other,
    )
    from_upper = lax.ppermute(upper, "yl", [(1, 0)])
    lower = call(
        lower_kernel, "lower", solved_shape, scratch,
        where, inverses, ring_rhs, from_upper, far_own, far_other, near_own, near_other,
    )
    solved = jnp.where(lax.axis_index("yl") == 1, upper, lower)
    spread = lax.all_to_all(
        solved.reshape(GROUPS, SUB, RING * NB), ("z", "yh"), 0, 0, tiled=True
    )[GROUPS - 1]
    count = lax.axis_size(ROWS)
    every = lax.all_to_all(
        jnp.broadcast_to(spread[None], (count, *spread.shape)), ROWS, 0, 0, tiled=True
    ).reshape(GROUPS, 2, RING * SUB, RING * NB)

    out = jax.ShapeDtypeStruct((NB, NB), jnp.float32)
    pending, image = call(
        final_kernel, "final", (out, out), [],
        where, every, own_w, other_w, own_z, other_z, rhs,
    )
    return pending.reshape(1, 1, NB, NB), image.reshape(1, 1, NB, NB)


def solution(mesh):
    fine = Mesh(mesh.devices.reshape(4, 2, 2, 4, 2), (*ROWS, "col"))
    wide = P(None, ROWS, None, None, "col", None)
    tall = P(None, ROWS, None, "col")
    return jax.shard_map(
        local, mesh=fine, in_specs=(wide, wide, wide, P(), P(), tall),
        out_specs=(tall, tall), check_vma=False,
    )
```

```python
import jax
import jax.numpy as jnp
from jax import lax
from jax.experimental import pallas as pl
from jax.experimental.pallas import tpu as pltpu
from jax.sharding import Mesh, PartitionSpec as P


STEPS = 8
HALF = STEPS // 2
NB = 256
RING = 4
SUB = 8
ROWS = ("z", "yh", "yl", "x")
GROUPS = 8
MINE = NB // RING


def times(a, b, **kw):
    return lax.dot_general(a, b, (((1,), (1,)), ((), ())), preferred_element_type=jnp.float32, **kw)


def halves(a):
    high = a.astype(jnp.bfloat16)
    return high, (a - high.astype(jnp.float32)).astype(jnp.bfloat16)


def precise(a, b):
    (a1, a2), (b1, b2) = halves(a), halves(b)
    return times(a1, b1) + (times(a2, b1) + times(a1, b2))


def back_substitute(where_ref, base, inv_ref, rhs, last, own_ref, other_ref, out_ref, x_ref):
    chip, parity = where_ref[0], where_ref[1]
    x_ref[...] = jnp.zeros_like(x_ref)
    for row in range(RING - 1, -1, -1):
        acc = rhs[row]
        if row == 0:
            acc = acc - last()
        if row < RING - 1:
            source = lax.rem(chip - row + RING, RING)
            for ref, p in ((other_ref, 1 - parity), (own_ref, parity)):
                acc = acc - times(x_ref[2 + p], ref[source])
        x = precise(acc, inv_ref[base + row]).astype(jnp.bfloat16)
        x_ref[row] = x
        out_ref[:, row * NB : (row + 1) * NB] = x


def upper_kernel(
    where_ref, inv_ref, rhs_ref, own_ref, other_ref, mid_own_ref, mid_other_ref, out_ref, x_ref
):
    chip, parity = where_ref[0], where_ref[1]
    rhs = [rhs_ref[lax.rem(chip - r + RING, RING)] for r in range(RING)]

    def last():
        return times(x_ref[parity], mid_own_ref[chip, 0]) + times(
            x_ref[1 - parity], mid_other_ref[chip, 0]
        )

    back_substitute(where_ref, RING, inv_ref, rhs, last, own_ref, other_ref, out_ref, x_ref)


def lower_kernel(
    where_ref, inv_ref, rhs_ref, solved_ref, far_own_ref, far_other_ref, mid_own_ref, mid_other_ref,
    near_ref, out_ref, x_ref, own_ref, other_ref,
):
    chip, parity = where_ref[0], where_ref[1]
    rhs = []
    for row in range(RING):
        source = lax.rem(chip - row + RING, RING)
        acc = rhs_ref[source]
        for own, p in ((False, 1 - parity), (True, parity)):
            near, far = (mid_own_ref, far_own_ref) if own else (mid_other_ref, far_other_ref)
            at = pl.multiple_of(p * NB, NB)
            acc = acc - times(solved_ref[:, pl.ds(at, NB)], near[source, 0])
            at = pl.multiple_of((2 + p) * NB, NB)
            acc = acc - times(solved_ref[:, pl.ds(at, NB)], far[source])
        rhs.append(acc)
        own_ref[source] = mid_own_ref[source, 1]
        other_ref[source] = mid_other_ref[source, 1]

    def last():
        return times(x_ref[1], near_ref[...])

    back_substitute(where_ref, 0, inv_ref, rhs, last, own_ref, other_ref, out_ref, x_ref)


def flip_kernel(rhs_ref, out_ref):
    flipped = rhs_ref[...].T
    for k in range(GROUPS):
        for x in range(RING):
            at = (k * RING + x) * SUB
            out_ref[x, k * SUB : (k + 1) * SUB] = flipped[at : at + SUB]


def final_kernel(
    where_ref, x_ref, w_own_ref, w_other_ref, z_own_ref, z_other_ref, rhs_ref, pending_ref, image_ref
):
    parity = where_ref[1]
    pending = rhs_ref[...]
    image = jnp.zeros_like(pending)
    for b in range(HALF):
        for w, z, p in ((w_own_ref, z_own_ref, parity), (w_other_ref, z_other_ref, 1 - parity)):
            at = pl.multiple_of((2 * (b % 2) + p) * NB, NB)
            x = x_ref[:, b // 2, :, pl.ds(at, NB)].reshape(NB, NB)
            pending = pending - times(w[b], x)
            image = image + times(z[b], x)
    pending_ref[...] = pending
    image_ref[...] = image


def call(kernel, outs, scratch, *args, limit=20 << 20):
    vmem = pl.BlockSpec(memory_space=pltpu.VMEM)
    smem = pl.BlockSpec(memory_space=pltpu.SMEM)
    return pl.pallas_call(
        kernel,
        out_shape=outs,
        in_specs=[smem if a.dtype == jnp.int32 else vmem for a in args],
        out_specs=jax.tree.map(lambda _: vmem, outs),
        scratch_shapes=scratch,
        compiler_params=pltpu.CompilerParams(vmem_limit_bytes=limit),
    )(*args)


def ring_sends(a, senders):
    out = []
    for s in range(1, RING):
        pairs = [
            ((yl * RING + x) * 2 + c, (yl * RING + (x + s) % RING) * 2 + c) for yl, x, c in senders
        ]
        out.append(lax.ppermute(a, ("yl", "x", "col"), pairs))
    return out


EVERY = [(yl, x, c) for yl in range(2) for x in range(RING) for c in range(2)]


def swapped(a):
    return lax.ppermute(a, "col", [(0, 1), (1, 0)])


def local(pencil_left, pencil_right, basis_panel, block_inverses, pencil_shift, start_vectors):
    row = lax.axis_index(ROWS)
    chip = lax.axis_index("x")
    parity = lax.axis_index("col")
    where = jnp.stack([chip, parity]).astype(jnp.int32)
    first = lax.axis_size(ROWS) - STEPS

    left = pencil_left.reshape(NB, HALF, NB)
    right = pencil_right.reshape(NB, HALF, NB)
    own_z = jnp.transpose(basis_panel.reshape(NB, HALF, NB), (1, 0, 2))
    rhs = start_vectors.reshape(NB, NB)
    inverses = block_inverses.reshape(STEPS, NB, NB)

    parts_shape = jax.ShapeDtypeStruct((RING, MINE, NB), jnp.float32)
    parts = call(flip_kernel, parts_shape, [], rhs)
    ring_rhs = []
    for s in range(1, RING):
        part = lax.dynamic_index_in_dim(parts, (chip + s) % RING, 0, keepdims=False)
        ring_rhs.append(lax.ppermute(part, "x", [(i, (i + s) % RING) for i in range(RING)]))
    mine = lax.dynamic_index_in_dim(parts, chip, 0, keepdims=False)

    cols = 2 * jnp.arange(HALF) + parity
    live = (row < first + cols)[None, :, None]
    both = left.astype(jnp.float32) - pencil_shift * right.astype(jnp.float32)
    own_w = jnp.transpose(jnp.where(live, both, 0.0).astype(jnp.bfloat16), (1, 0, 2))

    far = ring_sends(own_w[3], [e for e in EVERY if e[0] == 0 or e[1] < 3])
    mid = ring_sends(own_w[1:3][::-1], [e for e in EVERY if e[0] == 0 or e == (1, 0, 1)])
    near = ring_sends(own_w[0], [(0, 0, 1)])

    ring_rhs = jnp.stack([mine] + ring_rhs)
    far_own = jnp.stack([own_w[3]] + far)
    far_other = swapped(far_own)
    mid, far_own = lax.optimization_barrier((mid, far_own))
    mid_own = jnp.stack([own_w[1:3][::-1]] + mid)
    mid_other = swapped(mid_own)
    near_own = jnp.where(chip == 0, own_w[0], near[0] + near[1] + near[2])
    near_other = swapped(near_own)
    near_one = jnp.where(parity == 1, near_own, near_other)
    other_w = swapped(own_w)
    other_z = swapped(own_z)

    solved_shape = jax.ShapeDtypeStruct((MINE, RING * NB), jnp.bfloat16)
    solving = pltpu.VMEM((RING, MINE, NB), jnp.bfloat16)
    diagonal = pltpu.VMEM((RING, NB, NB), jnp.bfloat16)
    upper = call(
        upper_kernel, solved_shape, [solving],
        where, inverses, ring_rhs, far_own, far_other, mid_own, mid_other,
    )
    from_upper = lax.ppermute(upper, "yl", [(1, 0)])
    lower = call(
        lower_kernel, solved_shape, [solving, diagonal, diagonal],
        where, inverses, ring_rhs, from_upper, far_own, far_other, mid_own, mid_other, near_one,
    )
    solved = jnp.where(lax.axis_index("yl") == 1, upper, lower)
    spread = lax.all_to_all(
        solved.reshape(GROUPS, SUB, RING * NB), ("z", "yh"), 0, 0, tiled=True
    )[GROUPS - 1]
    count = lax.axis_size(ROWS)
    every = lax.all_to_all(
        jnp.broadcast_to(spread[None], (count, *spread.shape)), ROWS, 0, 0, tiled=True
    ).reshape(GROUPS, 2, RING * SUB, RING * NB)

    out = jax.ShapeDtypeStruct((NB, NB), jnp.float32)
    pending, image = call(
        final_kernel, (out, out), [],
        where, every, own_w, other_w, own_z, other_z, rhs,
    )
    return pending.reshape(1, 1, NB, NB), image.reshape(1, 1, NB, NB)


def solution(mesh):
    fine = Mesh(mesh.devices.reshape(4, 2, 2, 4, 2), (*ROWS, "col"))
    wide = P(None, ROWS, None, None, "col", None)
    tall = P(None, ROWS, None, "col")
    return jax.shard_map(
        local, mesh=fine, in_specs=(wide, wide, wide, P(), P(), tall),
        out_specs=(tall, tall), check_vma=False,
    )
```

```python
import functools

import jax
import jax.numpy as jnp
from jax import lax
from jax.experimental import pallas as pl
from jax.experimental.pallas import tpu as pltpu
from jax.sharding import Mesh, PartitionSpec as P


STEPS = 8
HALF = STEPS // 2
NB = 256
WIDE = NB // 2
GROUPS = 8
ROWS = ("z", "yh", "yl", "xp", "xq")
FLIP = [(0, 1), (1, 0)]


def dot(a, b):
    return jnp.dot(a, b, preferred_element_type=jnp.float32)


def halves(a):
    high = a.astype(jnp.bfloat16)
    return high, (a - high.astype(jnp.float32)).astype(jnp.bfloat16)


def precise(a, b):
    (a1, a2), (b1, b2) = halves(a), halves(b)
    return dot(a1, b1) + (dot(a2, b1) + dot(a1, b2))


def pair_kernel(
    turn, arriving, where_ref, inv_ref, rhs_ref, mate_rhs_ref, own_ref, other_ref,
    mate3_ref, mate3_other_ref, mate_ref, mate_other_ref, *rest,
):
    *arrived, prev_ref, out_ref, x_ref = rest
    pair, odd, half, parity = (where_ref[i] for i in range(4))

    def less(accs, b, x):
        own, mate = accs
        mine, theirs = x[parity], x[1 - parity]
        near = (mate3_ref[0], mate3_other_ref[0]) if b == HALF - 1 else (mate_ref[b], mate_other_ref[b])
        own = own - (dot(own_ref[b], mine) + dot(other_ref[b], theirs))
        return own, mate - (dot(near[0], mine) + dot(near[1], theirs))

    @pl.when(pair == turn)
    def _():
        accs = rhs_ref[:, pl.ds(pl.multiple_of(half * WIDE, WIDE), WIDE)], mate_rhs_ref[...]
        for b, x in zip(arriving, arrived):
            accs = less(accs, b, x)
        high = jnp.where(odd == 1, *accs)
        x_high = precise(inv_ref[2 * turn + 1], high).astype(jnp.bfloat16)
        x_ref[0] = jnp.zeros_like(x_high)
        x_ref[1] = x_high
        accs = less(accs, turn, x_ref)
        low = jnp.where(odd == 0, *accs)
        out_ref[0] = precise(inv_ref[2 * turn], low).astype(jnp.bfloat16)
        out_ref[1] = x_high

    @pl.when(pair != turn)
    def _():
        out_ref[...] = prev_ref[...]


def final_kernel(
    where_ref, x_ref, w_own_ref, w_other_ref, z_own_ref, z_other_ref, rhs_ref, pending_ref, image_ref
):
    parity = where_ref[3]
    pending = rhs_ref[...]
    image = jnp.zeros_like(pending)
    for b in range(HALF):
        yl, xp = b // 2, b % 2
        for w, z, p in ((w_own_ref, z_own_ref, parity), (w_other_ref, z_other_ref, 1 - parity)):
            columns = []
            for half in range(2):
                at = [(((4 * p + i) * 2 + yl) * 2 + xp) * 2 + (half ^ xp) for i in range(4)]
                columns.append(jnp.concatenate([x_ref[n] for n in at], 0))
            x = jnp.concatenate(columns, 1)
            pending = pending - dot(w[b], x)
            image = image + dot(z[b], x)
    pending_ref[...] = pending
    image_ref[...] = image


def call(kernel, outs, scratch, *args, limit=24 << 20):
    vmem = pl.BlockSpec(memory_space=pltpu.VMEM)
    smem = pl.BlockSpec(memory_space=pltpu.SMEM)
    return pl.pallas_call(
        kernel,
        out_shape=outs,
        in_specs=[smem if a.dtype == jnp.int32 else vmem for a in args],
        out_specs=jax.tree.map(lambda _: vmem, outs),
        scratch_shapes=scratch,
        compiler_params=pltpu.CompilerParams(vmem_limit_bytes=limit),
    )(*args)


def to_pairs(a, moves):
    sends = []
    for src, dst in moves:
        for half in range(2):
            sends.append(tuple(2 * m + (half ^ (m % 2)) for m in (src, dst)))
    return lax.ppermute(a, ("yl", "xp", "xq"), sends)


def local(pencil_left, pencil_right, basis_panel, block_inverses, pencil_shift, start_vectors):
    row = lax.axis_index(ROWS)
    parity = lax.axis_index("col")
    pair = lax.axis_index(("yl", "xp"))
    odd = lax.axis_index("xq")
    half = odd ^ lax.axis_index("xp")
    where = jnp.stack([pair, odd, half, parity]).astype(jnp.int32)
    first = lax.axis_size(ROWS) - STEPS

    left = pencil_left.reshape(NB, HALF, NB)
    right = pencil_right.reshape(NB, HALF, NB)
    own_z = jnp.transpose(basis_panel.reshape(NB, HALF, NB), (1, 0, 2))
    rhs = start_vectors.reshape(NB, NB)
    inverses = block_inverses.reshape(STEPS, NB, NB)

    their_half = lax.dynamic_slice_in_dim(rhs, (1 - half) * WIDE, WIDE, 1)
    mate_rhs = lax.ppermute(their_half, "xq", FLIP)

    cols = 2 * jnp.arange(HALF) + parity
    live = (row < first + cols)[None, :, None]
    both = left.astype(jnp.float32) - pencil_shift * right.astype(jnp.float32)
    own_w = jnp.transpose(jnp.where(live, both, 0.0).astype(jnp.bfloat16), (1, 0, 2))

    mate3 = lax.ppermute(own_w[HALF - 1 :], "xq", FLIP)
    other_w = lax.ppermute(own_w, "col", FLIP)
    mate = lax.ppermute(own_w[: HALF - 1], "xq", FLIP)
    mate3_other = lax.ppermute(mate3, "col", FLIP)
    mate_other = lax.ppermute(mate, "col", FLIP)
    other_z = lax.ppermute(own_z, "col", FLIP)

    shape = jax.ShapeDtypeStruct((2, NB, WIDE), jnp.bfloat16)
    scratch = [pltpu.VMEM((2, NB, WIDE), jnp.bfloat16)]

    def solve(turn, arrivals, prev):
        return call(
            functools.partial(pair_kernel, turn, [b for b, _ in arrivals]), shape, scratch,
            where, inverses, rhs, mate_rhs, own_w, other_w, mate3, mate3_other,
            *((mate, mate_other) if turn < 3 else (mate3, mate3_other)),
            *[x for _, x in arrivals], prev,
        )

    x3 = solve(3, [], jnp.zeros(shape.shape, shape.dtype))
    a = to_pairs(x3, [(3, 2)])
    b = to_pairs(x3, [(3, 1)])
    x2 = solve(2, [(3, a)], x3)
    c = to_pairs(x2, [(2, 1), (3, 0)])
    d = to_pairs(x2, [(2, 0)])
    x1 = solve(1, [(3, b), (2, c)], x2)
    e = to_pairs(x1, [(1, 0)])
    x0 = solve(0, [(3, c), (2, d), (1, e)], x1)

    spread = lax.all_to_all(
        x0.reshape(GROUPS, 2 * NB // GROUPS, WIDE), ("z", "yh"), 0, 0, tiled=True
    )[GROUPS - 1]
    count = lax.axis_size(ROWS)
    every = lax.all_to_all(
        jnp.broadcast_to(spread[None], (count, *spread.shape)), ROWS, 0, 0, tiled=True
    )

    out = jax.ShapeDtypeStruct((NB, NB), jnp.float32)
    pending, image = call(
        final_kernel, (out, out), [],
        where, every, own_w, other_w, own_z, other_z, rhs,
    )
    return pending.reshape(1, 1, NB, NB), image.reshape(1, 1, NB, NB)


def solution(mesh):
    fine = Mesh(mesh.devices.reshape(4, 2, 2, 2, 2, 2), (*ROWS, "col"))
    wide = P(None, ROWS, None, None, "col", None)
    tall = P(None, ROWS, None, "col")
    return jax.shard_map(
        local, mesh=fine, in_specs=(wide, wide, wide, P(), P(), tall),
        out_specs=(tall, tall), check_vma=False,
    )
```

```python
import functools

import jax
import jax.numpy as jnp
from jax import lax
from jax.experimental import pallas as pl
from jax.experimental.pallas import tpu as pltpu
from jax.sharding import Mesh, PartitionSpec as P


STEPS = 8
HALF = STEPS // 2
NB = 256
WIDE = NB // 2
GROUPS = 8
ROWS = ("z", "yh", "yl", "xp", "xq")
FLIP = [(0, 1), (1, 0)]


def dot(a, b):
    return jnp.dot(a, b, preferred_element_type=jnp.float32)


def halves(a):
    high = a.astype(jnp.bfloat16)
    return high, (a - high.astype(jnp.float32)).astype(jnp.bfloat16)


def lead_kernel(where_ref, inv_ref, rhs_ref, inv_out_ref, rhs_out_ref):
    pair, half = where_ref[0], where_ref[2]
    rhs_out_ref[...] = jnp.where(half == 0, rhs_ref[:, WIDE:], rhs_ref[:, :WIDE])
    for e in range(2):
        inv_out_ref[e, 0], inv_out_ref[e, 1] = halves(inv_ref[pair, e])


def precise(inv_ref, e, b):
    high, low = halves(b)
    return dot(inv_ref[e, 0], high) + (dot(inv_ref[e, 1], high) + dot(inv_ref[e, 0], low))


def pair_kernel(
    turn, arriving, early, where_ref, inv_ref, rhs_ref, mate_rhs_ref,
    own_ref, other3_ref, mate3_ref, mate3_other_ref, *rest,
):
    if turn < HALF - 1:
        other_ref, mate_ref, mate_other_ref, *rest = rest
    *seen, acc_ref, prev_ref, out_ref, sum_ref = rest
    pair, odd, half, parity = (where_ref[i] for i in range(4))

    def blocks(b):
        if b == HALF - 1:
            return own_ref[b], other3_ref[0], mate3_ref[0], mate3_other_ref[0]
        return own_ref[b], other_ref[b], mate_ref[b], mate_other_ref[b]

    def less(accs, b, x):
        own, other, mate, mate_other = blocks(b)
        mine, theirs = x[parity], x[1 - parity]
        return (
            accs[0] - (dot(own, mine) + dot(other, theirs)),
            accs[1] - (dot(mate, mine) + dot(mate_other, theirs)),
        )

    def fresh():
        return rhs_ref[:, pl.ds(pl.multiple_of(half * WIDE, WIDE), WIDE)], mate_rhs_ref[...]

    @pl.when(pair == turn)
    def _():
        accs = fresh() if turn >= HALF - 2 else (acc_ref[0], acc_ref[1])
        for b, x in zip(arriving, seen):
            accs = less(accs, b, x)
        high = jnp.where(odd == 1, *accs)
        own, other, mate, mate_other = blocks(turn)
        between = jnp.where(
            odd == 0, jnp.where(parity == 1, own, other), jnp.where(parity == 1, mate, mate_other)
        )
        x_high = precise(inv_ref, 1, high).astype(jnp.bfloat16)
        low = jnp.where(odd == 0, *accs) - dot(between, x_high)
        out_ref[0] = precise(inv_ref, 0, low).astype(jnp.bfloat16)
        out_ref[1] = x_high

    @pl.when(pair != turn)
    def _():
        out_ref[...] = prev_ref[...]

    @pl.when(pair == turn - 1)
    def _():
        accs = fresh()
        for b, x in zip(early, seen[len(arriving) :]):
            accs = less(accs, b, x)
        sum_ref[0], sum_ref[1] = accs


def final_kernel(
    where_ref, x_ref, w_own_ref, w3_other_ref, w_other_ref, z_own_ref, z_other_ref,
    rhs_ref, pending_ref, image_ref,
):
    parity = where_ref[3]
    pending = rhs_ref[...]
    image = jnp.zeros_like(pending)
    for b in range(HALF):
        yl, xp = b // 2, b % 2
        own, other = w_own_ref[b], w3_other_ref[0] if b == HALF - 1 else w_other_ref[b]
        for w, z, p in ((own, z_own_ref, parity), (other, z_other_ref, 1 - parity)):
            columns = []
            for half in range(2):
                at = [(((4 * p + i) * 2 + yl) * 2 + xp) * 2 + (half ^ xp) for i in range(4)]
                columns.append(jnp.concatenate([x_ref[n] for n in at], 0))
            x = jnp.concatenate(columns, 1)
            pending = pending - dot(w, x)
            image = image + dot(z[b], x)
    pending_ref[...] = pending
    image_ref[...] = image


def call(kernel, outs, scratch, *args, limit=12 << 20):
    vmem = pl.BlockSpec(memory_space=pltpu.VMEM)
    smem = pl.BlockSpec(memory_space=pltpu.SMEM)
    return pl.pallas_call(
        kernel,
        out_shape=outs,
        in_specs=[smem if a.dtype == jnp.int32 else vmem for a in args],
        out_specs=jax.tree.map(lambda _: vmem, outs),
        scratch_shapes=scratch,
        compiler_params=pltpu.CompilerParams(vmem_limit_bytes=limit),
    )(*args)


def to_pairs(a, moves):
    sends = []
    for src, dst in moves:
        for half in range(2):
            sends.append(tuple(2 * m + (half ^ (m % 2)) for m in (src, dst)))
    return lax.ppermute(a, ("yl", "xp", "xq"), sends)


def local(pencil_left, pencil_right, basis_panel, block_inverses, pencil_shift, start_vectors):
    row = lax.axis_index(ROWS)
    parity = lax.axis_index("col")
    pair = lax.axis_index(("yl", "xp"))
    odd = lax.axis_index("xq")
    half = odd ^ lax.axis_index("xp")
    where = jnp.stack([pair, odd, half, parity]).astype(jnp.int32)
    where, pencil_shift = lax.optimization_barrier((where, pencil_shift))
    first = lax.axis_size(ROWS) - STEPS

    left = pencil_left.reshape(NB, HALF, NB)
    right = pencil_right.reshape(NB, HALF, NB)
    own_z = jnp.transpose(basis_panel.reshape(NB, HALF, NB), (1, 0, 2))
    rhs = start_vectors.reshape(NB, NB)

    cols = 2 * jnp.arange(HALF) + parity
    live = (row < first + cols)[None, :, None]
    both = left.astype(jnp.float32) - pencil_shift * right.astype(jnp.float32)
    own = jnp.transpose(jnp.where(live, both, 0.0).astype(jnp.bfloat16), (1, 0, 2))
    own3 = own[HALF - 1 :]
    mate3 = lax.ppermute(own3, "xq", FLIP)
    other3 = lax.ppermute(own3, "col", FLIP)
    lead_shapes = (
        jax.ShapeDtypeStruct((2, 2, NB, NB), jnp.bfloat16), jax.ShapeDtypeStruct((NB, WIDE), jnp.float32)
    )
    inverses, their_rhs = call(lead_kernel, lead_shapes, [], where, block_inverses, rhs)
    mate_rhs = lax.ppermute(their_rhs, "xq", FLIP)
    mate3_other = lax.ppermute(mate3, "col", FLIP)
    lower = own[: HALF - 1]
    mate = lax.ppermute(lower, "xq", FLIP)
    other = lax.ppermute(lower, "col", FLIP)
    mate_other = lax.ppermute(mate, "col", FLIP)
    other_z = lax.ppermute(own_z, "col", FLIP)

    shape = jax.ShapeDtypeStruct((2, NB, WIDE), jnp.bfloat16)
    sums = jax.ShapeDtypeStruct((2, NB, WIDE), jnp.float32)

    def solve(turn, arriving, early, acc, prev):
        return call(
            functools.partial(pair_kernel, turn, [b for b, _ in arriving], [b for b, _ in early]),
            (shape, sums), [],
            where, inverses, rhs, mate_rhs, own, other3, mate3, mate3_other,
            *((other, mate, mate_other) if turn < HALF - 1 else ()),
            *[x for _, x in arriving + early], acc, prev,
        )

    x3, acc = solve(3, [], [], jnp.zeros(sums.shape, sums.dtype), jnp.zeros(shape.shape, shape.dtype))
    a = to_pairs(x3, [(3, 2)])
    b = to_pairs(x3, [(3, 1)])
    x2, acc = solve(2, [(3, a)], [(3, b)], acc, x3)
    c = to_pairs(x2, [(2, 1), (3, 0)])
    d = to_pairs(x2, [(2, 0)])
    x1, acc = solve(1, [(2, c)], [(3, c), (2, d)], acc, x2)
    e = to_pairs(x1, [(1, 0)])
    x0, _ = solve(0, [(1, e)], [], acc, x1)

    spread = lax.all_to_all(
        x0.reshape(GROUPS, 2 * NB // GROUPS, WIDE), ("z", "yh"), 0, 0, tiled=True
    )[GROUPS - 1]
    spread, other_z, other, other3, own_z = lax.optimization_barrier((spread, other_z, other, other3, own_z))
    count = lax.axis_size(ROWS)
    every = lax.all_to_all(
        jnp.broadcast_to(spread[None], (count, *spread.shape)), ROWS, 0, 0, tiled=True
    )

    out = jax.ShapeDtypeStruct((NB, NB), jnp.float32)
    pending, image = call(
        final_kernel, (out, out), [],
        where, every, own, other3, other, own_z, other_z, rhs,
    )
    return pending.reshape(1, 1, NB, NB), image.reshape(1, 1, NB, NB)


def solution(mesh):
    fine = Mesh(mesh.devices.reshape(4, 2, 2, 2, 2, 2), (*ROWS, "col"))
    wide = P(None, ROWS, None, None, "col", None)
    tall = P(None, ROWS, None, "col")
    return jax.shard_map(
        local, mesh=fine, in_specs=(wide, wide, wide, P(), P(), tall),
        out_specs=(tall, tall), check_vma=False,
    )
```

```python
import functools

import jax
import jax.numpy as jnp
from jax import lax
from jax.experimental import pallas as pl
from jax.experimental.pallas import tpu as pltpu
from jax.sharding import Mesh, PartitionSpec as P


STEPS = 8
HALF = STEPS // 2
NB = 256
WIDE = NB // 2
GROUPS = 8
ROWS = ("z", "yh", "yl", "xp", "xq")
FLIP = [(0, 1), (1, 0)]


def dot(a, b):
    return jnp.dot(a, b, preferred_element_type=jnp.float32)


def halves(a):
    high = a.astype(jnp.bfloat16)
    return high, (a - high.astype(jnp.float32)).astype(jnp.bfloat16)


def split_kernel(where_ref, inv_ref, out_ref):
    for e in range(2):
        out_ref[e, 0], out_ref[e, 1] = halves(inv_ref[where_ref[0], e])


def precise(inv_ref, e, b):
    high, low = halves(b)
    return dot(inv_ref[e, 0], high) + (dot(inv_ref[e, 1], high) + dot(inv_ref[e, 0], low))


def pair_kernel(
    turn, arriving, early, where_ref, inv_ref, rhs_ref, mate_rhs_ref, own_ref, *rest,
):
    groups = min(HALF - turn, 3)
    foreign, rest = rest[: 3 * groups], rest[3 * groups :]
    if turn:
        *seen, acc_ref, prev_ref, out_ref, sum_ref = rest
    else:
        *seen, acc_ref, prev_ref, out_ref = rest
    pair, odd, half, parity = (where_ref[i] for i in range(4))

    def blocks(b):
        n, at = max(HALF - 1 - b, 0), 0
        if n >= 2:
            n, at = 2, b
        return own_ref[b], *(ref[at] for ref in foreign[3 * n : 3 * n + 3])

    def less(accs, b, x):
        own, other, mate, mate_other = blocks(b)
        mine, theirs = x[parity], x[1 - parity]
        return (
            accs[0] - (dot(own, mine) + dot(other, theirs)),
            accs[1] - (dot(mate, mine) + dot(mate_other, theirs)),
        )

    def fresh():
        return rhs_ref[:, pl.ds(pl.multiple_of(half * WIDE, WIDE), WIDE)], mate_rhs_ref[...]

    @pl.when(pair == turn)
    def _():
        accs = fresh() if turn >= HALF - 2 else (acc_ref[0], acc_ref[1])
        for b, x in zip(arriving, seen):
            accs = less(accs, b, x)
        high = jnp.where(odd == 1, *accs)
        own, other, mate, mate_other = blocks(turn)
        between = jnp.where(
            odd == 0, jnp.where(parity == 1, own, other), jnp.where(parity == 1, mate, mate_other)
        )
        x_high = precise(inv_ref, 1, high).astype(jnp.bfloat16)
        low = jnp.where(odd == 0, *accs) - dot(between, x_high)
        out_ref[0] = precise(inv_ref, 0, low).astype(jnp.bfloat16)
        out_ref[1] = x_high

    @pl.when(pair != turn)
    def _():
        out_ref[...] = prev_ref[...]

    if turn:
        @pl.when(pair == turn - 1)
        def _():
            accs = fresh()
            for b, x in zip(early, seen[len(arriving) :]):
                accs = less(accs, b, x)
            sum_ref[0], sum_ref[1] = accs


def final_kernel(
    where_ref, x_ref, w_own_ref, other3_ref, other2_ref, other01_ref, z_own_ref, z_other_ref,
    rhs_ref, pending_ref, image_ref,
):
    parity = where_ref[3]
    pending = rhs_ref[...]
    image = jnp.zeros_like(pending)
    for b in range(HALF):
        yl, xp = b // 2, b % 2
        own, other = w_own_ref[b], (other01_ref[b] if b < 2 else (other2_ref, other3_ref)[b - 2][0])
        for w, z, p in ((own, z_own_ref, parity), (other, z_other_ref, 1 - parity)):
            columns = []
            for half in range(2):
                at = [(((4 * p + i) * 2 + yl) * 2 + xp) * 2 + (half ^ xp) for i in range(4)]
                columns.append(jnp.concatenate([x_ref[n] for n in at], 0))
            x = jnp.concatenate(columns, 1)
            pending = pending - dot(w, x)
            image = image + dot(z[b], x)
    pending_ref[...] = pending
    image_ref[...] = image


def call(kernel, outs, scratch, *args, limit=12 << 20):
    vmem = pl.BlockSpec(memory_space=pltpu.VMEM)
    smem = pl.BlockSpec(memory_space=pltpu.SMEM)
    return pl.pallas_call(
        kernel,
        out_shape=outs,
        in_specs=[smem if a.dtype == jnp.int32 else vmem for a in args],
        out_specs=jax.tree.map(lambda _: vmem, outs),
        scratch_shapes=scratch,
        compiler_params=pltpu.CompilerParams(vmem_limit_bytes=limit),
    )(*args)


def to_pairs(a, moves):
    sends = []
    for src, dst in moves:
        for half in range(2):
            sends.append(tuple(2 * m + (half ^ (m % 2)) for m in (src, dst)))
    return lax.ppermute(a, ("yl", "xp", "xq"), sends)


def local(pencil_left, pencil_right, basis_panel, block_inverses, pencil_shift, start_vectors):
    row = lax.axis_index(ROWS)
    parity = lax.axis_index("col")
    pair = lax.axis_index(("yl", "xp"))
    odd = lax.axis_index("xq")
    half = odd ^ lax.axis_index("xp")
    where = jnp.stack([pair, odd, half, parity]).astype(jnp.int32)
    where, pencil_shift, lower_half = lax.optimization_barrier((where, pencil_shift, half == 0))
    first = lax.axis_size(ROWS) - STEPS

    left = pencil_left.reshape(NB, HALF, NB)
    right = pencil_right.reshape(NB, HALF, NB)
    own_z = jnp.transpose(basis_panel.reshape(NB, HALF, NB), (1, 0, 2))
    rhs = start_vectors.reshape(NB, NB)

    cols = 2 * jnp.arange(HALF) + parity
    live = (row < first + cols)[None, :, None]
    both = left.astype(jnp.float32) - pencil_shift * right.astype(jnp.float32)
    own = jnp.transpose(jnp.where(live, both, 0.0).astype(jnp.bfloat16), (1, 0, 2))
    own3 = own[HALF - 1 :]
    mate3 = lax.ppermute(own3, "xq", FLIP)
    other3 = lax.ppermute(own3, "col", FLIP)
    mate_rhs = lax.ppermute(jnp.where(lower_half, rhs[:, WIDE:], rhs[:, :WIDE]), "xq", FLIP)
    mate3_other = lax.ppermute(mate3, "col", FLIP)
    mate2 = lax.ppermute(own[2:3], "xq", FLIP)
    other2 = lax.ppermute(own[2:3], "col", FLIP)
    inverses = call(
        split_kernel, jax.ShapeDtypeStruct((2, 2, NB, NB), jnp.bfloat16), [], where, block_inverses
    )
    mate01 = lax.ppermute(own[:2], "xq", FLIP)
    other01 = lax.ppermute(own[:2], "col", FLIP)
    mate2_other = lax.ppermute(mate2, "col", FLIP)
    mate01_other = lax.ppermute(mate01, "col", FLIP)
    other_z = lax.ppermute(own_z, "col", FLIP)

    shape = jax.ShapeDtypeStruct((2, NB, WIDE), jnp.bfloat16)
    sums = jax.ShapeDtypeStruct((2, NB, WIDE), jnp.float32)

    foreign = (
        (other3, mate3, mate3_other), (other2, mate2, mate2_other), (other01, mate01, mate01_other)
    )

    def solve(turn, arriving, early, acc, prev):
        return call(
            functools.partial(pair_kernel, turn, [b for b, _ in arriving], [b for b, _ in early]),
            (shape, sums) if turn else shape, [],
            where, inverses, rhs, mate_rhs, own, *sum(foreign[: HALF - turn], ()),
            *[x for _, x in arriving + early], acc, prev,
        )

    x3, acc = solve(3, [], [], jnp.zeros(sums.shape, sums.dtype), jnp.zeros(shape.shape, shape.dtype))
    a = to_pairs(x3, [(3, 2)])
    b = to_pairs(x3, [(3, 1)])
    x2, acc = solve(2, [(3, a)], [(3, b)], acc, x3)
    c = to_pairs(x2, [(2, 1), (3, 0)])
    d = to_pairs(x2, [(2, 0)])
    x1, acc = solve(1, [(2, c)], [(3, c), (2, d)], acc, x2)
    e = to_pairs(x1, [(1, 0)])
    x0 = solve(0, [(1, e)], [], acc, x1)

    spread = lax.all_to_all(
        x0.reshape(GROUPS, 2 * NB // GROUPS, WIDE), ("z", "yh"), 0, 0, tiled=True
    )[GROUPS - 1]
    spread, other_z = lax.optimization_barrier((spread, other_z))
    count = lax.axis_size(ROWS)
    every = lax.all_to_all(
        jnp.broadcast_to(spread[None], (count, *spread.shape)), ROWS, 0, 0, tiled=True
    )

    out = jax.ShapeDtypeStruct((NB, NB), jnp.float32)
    pending, image = call(
        final_kernel, (out, out), [],
        where, every, own, other3, other2, other01, own_z, other_z, rhs,
    )
    return pending.reshape(1, 1, NB, NB), image.reshape(1, 1, NB, NB)


def solution(mesh):
    fine = Mesh(mesh.devices.reshape(4, 2, 2, 2, 2, 2), (*ROWS, "col"))
    wide = P(None, ROWS, None, None, "col", None)
    tall = P(None, ROWS, None, "col")
    return jax.shard_map(
        local, mesh=fine, in_specs=(wide, wide, wide, P(), P(), tall),
        out_specs=(tall, tall), check_vma=False,
    )
```

```python
import functools

import jax
import jax.numpy as jnp
from jax import lax
from jax.experimental import pallas as pl
from jax.experimental.pallas import tpu as pltpu
from jax.sharding import Mesh, PartitionSpec as P


STEPS = 8
HALF = STEPS // 2
NB = 256
WIDE = NB // 2
GROUPS = 8
ROWS = ("z", "yh", "yl", "xp", "xq")
FLIP = [(0, 1), (1, 0)]


def dot(a, b):
    return jnp.dot(a, b, preferred_element_type=jnp.float32)


def halves(a):
    high = a.astype(jnp.bfloat16)
    return high, (a - high.astype(jnp.float32)).astype(jnp.bfloat16)


def split_kernel(where_ref, inv_ref, out_ref):
    for e in range(2):
        out_ref[e, 0], out_ref[e, 1] = halves(inv_ref[where_ref[0], e])


def precise(inv_ref, e, b):
    high, low = halves(b)
    return dot(inv_ref[e, 0], high) + (dot(inv_ref[e, 1], high) + dot(inv_ref[e, 0], low))


def pair_kernel(
    turn, arriving, early, where_ref, inv_ref, rhs_ref, mate_rhs_ref, own_ref, *rest,
):
    groups = min(HALF - turn, 3)
    foreign, rest = rest[: 3 * groups], rest[3 * groups :]
    seen, rest = rest[: len(arriving) + len(early)], rest[len(arriving) + len(early) :]
    acc_ref = None if turn else rest[0]
    prev_ref, out_ref = rest[-3:-1] if early else rest[-2:]
    sum_ref = rest[-1] if early else None
    pair, odd, half, parity = (where_ref[i] for i in range(4))

    def blocks(b):
        n, at = max(HALF - 1 - b, 0), 0
        if n >= 2:
            n, at = 2, b
        return own_ref[b], *(ref[at] for ref in foreign[3 * n : 3 * n + 3])

    def less(accs, b, x):
        own, other, mate, mate_other = blocks(b)
        mine, theirs = x[parity], x[1 - parity]
        return (
            accs[0] - (dot(own, mine) + dot(other, theirs)),
            accs[1] - (dot(mate, mine) + dot(mate_other, theirs)),
        )

    def fresh():
        return rhs_ref[:, pl.ds(pl.multiple_of(half * WIDE, WIDE), WIDE)], mate_rhs_ref[...]

    @pl.when(pair == turn)
    def _():
        accs = fresh() if turn else (acc_ref[0], acc_ref[1])
        for b, x in zip(arriving, seen):
            accs = less(accs, b, x)
        high = jnp.where(odd == 1, *accs)
        own, other, mate, mate_other = blocks(turn)
        between = jnp.where(
            odd == 0, jnp.where(parity == 1, own, other), jnp.where(parity == 1, mate, mate_other)
        )
        x_high = precise(inv_ref, 1, high).astype(jnp.bfloat16)
        low = jnp.where(odd == 0, *accs) - dot(between, x_high)
        out_ref[0] = precise(inv_ref, 0, low).astype(jnp.bfloat16)
        out_ref[1] = x_high

    @pl.when(pair != turn)
    def _():
        out_ref[...] = prev_ref[...]

    if early:
        @pl.when(pair == turn - 1)
        def _():
            accs = fresh()
            for b, x in zip(early, seen[len(arriving) :]):
                accs = less(accs, b, x)
            sum_ref[0], sum_ref[1] = accs


def final_kernel(
    where_ref, x_ref, w_own_ref, other3_ref, other2_ref, other01_ref, z_own_ref, z_other_ref,
    rhs_ref, pending_ref, image_ref,
):
    parity = where_ref[3]
    pending = rhs_ref[...]
    image = jnp.zeros_like(pending)
    for b in range(HALF):
        yl, xp = b // 2, b % 2
        own, other = w_own_ref[b], (other01_ref[b] if b < 2 else (other2_ref, other3_ref)[b - 2][0])
        for w, z, p in ((own, z_own_ref, parity), (other, z_other_ref, 1 - parity)):
            columns = []
            for half in range(2):
                at = [(((4 * p + i) * 2 + yl) * 2 + xp) * 2 + (half ^ xp) for i in range(4)]
                columns.append(jnp.concatenate([x_ref[n] for n in at], 0))
            x = jnp.concatenate(columns, 1)
            pending = pending - dot(w, x)
            image = image + dot(z[b], x)
    pending_ref[...] = pending
    image_ref[...] = image


def call(kernel, outs, scratch, *args, limit=12 << 20):
    vmem = pl.BlockSpec(memory_space=pltpu.VMEM)
    smem = pl.BlockSpec(memory_space=pltpu.SMEM)
    return pl.pallas_call(
        kernel,
        out_shape=outs,
        in_specs=[smem if a.dtype == jnp.int32 else vmem for a in args],
        out_specs=jax.tree.map(lambda _: vmem, outs),
        scratch_shapes=scratch,
        compiler_params=pltpu.CompilerParams(vmem_limit_bytes=limit),
    )(*args)


def to_pairs(a, moves):
    sends = []
    for src, dst in moves:
        for half in range(2):
            sends.append(tuple(2 * m + (half ^ (m % 2)) for m in (src, dst)))
    return lax.ppermute(a, ("yl", "xp", "xq"), sends)


def local(pencil_left, pencil_right, basis_panel, block_inverses, pencil_shift, start_vectors):
    row = lax.axis_index(ROWS)
    parity = lax.axis_index("col")
    pair = lax.axis_index(("yl", "xp"))
    odd = lax.axis_index("xq")
    half = odd ^ lax.axis_index("xp")
    where = jnp.stack([pair, odd, half, parity]).astype(jnp.int32)
    where, pencil_shift, lower_half = lax.optimization_barrier((where, pencil_shift, half == 0))
    first = lax.axis_size(ROWS) - STEPS

    left = pencil_left.reshape(NB, HALF, NB)
    right = pencil_right.reshape(NB, HALF, NB)
    own_z = jnp.transpose(basis_panel.reshape(NB, HALF, NB), (1, 0, 2))
    rhs = start_vectors.reshape(NB, NB)

    cols = 2 * jnp.arange(HALF) + parity
    live = (row < first + cols)[None, :, None]
    both = left.astype(jnp.float32) - pencil_shift * right.astype(jnp.float32)
    own = jnp.transpose(jnp.where(live, both, 0.0).astype(jnp.bfloat16), (1, 0, 2))
    own3 = own[HALF - 1 :]
    mate3 = lax.ppermute(own3, "xq", FLIP)
    other3 = lax.ppermute(own3, "col", FLIP)
    mate_rhs = lax.ppermute(jnp.where(lower_half, rhs[:, WIDE:], rhs[:, :WIDE]), "xq", FLIP)
    mate3_other = lax.ppermute(mate3, "col", FLIP)
    mate2 = lax.ppermute(own[2:3], "xq", FLIP)
    other2 = lax.ppermute(own[2:3], "col", FLIP)
    inverses = call(
        split_kernel, jax.ShapeDtypeStruct((2, 2, NB, NB), jnp.bfloat16), [], where, block_inverses
    )
    mate01 = lax.ppermute(own[:2], "xq", FLIP)
    other01 = lax.ppermute(own[:2], "col", FLIP)
    mate2_other = lax.ppermute(mate2, "col", FLIP)
    mate01_other = lax.ppermute(mate01, "col", FLIP)
    other_z = lax.ppermute(own_z, "col", FLIP)

    shape = jax.ShapeDtypeStruct((2, NB, WIDE), jnp.bfloat16)
    sums = jax.ShapeDtypeStruct((2, NB, WIDE), jnp.float32)

    foreign = (
        (other3, mate3, mate3_other), (other2, mate2, mate2_other), (other01, mate01, mate01_other)
    )

    def solve(turn, arriving, early, *last):
        return call(
            functools.partial(pair_kernel, turn, [b for b, _ in arriving], [b for b, _ in early]),
            (shape, sums) if early else shape, [],
            where, inverses, rhs, mate_rhs, own, *sum(foreign[: HALF - turn], ()),
            *[x for _, x in arriving + early], *last,
        )

    x3 = solve(3, [], [], jnp.zeros(shape.shape, shape.dtype))
    a = to_pairs(x3, [(3, 2)])
    b = to_pairs(x3, [(3, 1)])
    x2 = solve(2, [(3, a)], [], x3)
    c = to_pairs(x2, [(2, 1), (3, 0)])
    d = to_pairs(x2, [(2, 0)])
    x1, acc = solve(1, [(3, b), (2, c)], [(3, c), (2, d)], x2)
    e = to_pairs(x1, [(1, 0)])
    x0 = solve(0, [(1, e)], [], acc, x1)

    spread = lax.all_to_all(
        x0.reshape(GROUPS, 2 * NB // GROUPS, WIDE), ("z", "yh"), 0, 0, tiled=True
    )[GROUPS - 1]
    spread, other_z = lax.optimization_barrier((spread, other_z))
    count = lax.axis_size(ROWS)
    every = lax.all_to_all(
        jnp.broadcast_to(spread[None], (count, *spread.shape)), ROWS, 0, 0, tiled=True
    )

    out = jax.ShapeDtypeStruct((NB, NB), jnp.float32)
    pending, image = call(
        final_kernel, (out, out), [],
        where, every, own, other3, other2, other01, own_z, other_z, rhs,
    )
    return pending.reshape(1, 1, NB, NB), image.reshape(1, 1, NB, NB)


def solution(mesh):
    fine = Mesh(mesh.devices.reshape(4, 2, 2, 2, 2, 2), (*ROWS, "col"))
    wide = P(None, ROWS, None, None, "col", None)
    tall = P(None, ROWS, None, "col")
    return jax.shard_map(
        local, mesh=fine, in_specs=(wide, wide, wide, P(), P(), tall),
        out_specs=(tall, tall), check_vma=False,
    )
```

```python
import functools

import jax
import jax.numpy as jnp
from jax import lax
from jax.experimental import pallas as pl
from jax.experimental.pallas import tpu as pltpu
from jax.sharding import Mesh, PartitionSpec as P


STEPS = 8
HALF = STEPS // 2
NB = 256
WIDE = NB // 2
GROUPS = 8
ROWS = ("z", "yh", "yl", "xp", "xq")
FLIP = [(0, 1), (1, 0)]


def dot(a, b):
    return jnp.dot(a, b, preferred_element_type=jnp.float32)


def halves(a):
    high = a.astype(jnp.bfloat16)
    return high, (a - high.astype(jnp.float32)).astype(jnp.bfloat16)


def split_kernel(where_ref, inv_ref, out_ref):
    for e in range(2):
        out_ref[e, 0], out_ref[e, 1] = halves(inv_ref[where_ref[0], e])


def precise(inv_ref, e, b):
    high, low = halves(b)
    return dot(inv_ref[e, 0], high) + (dot(inv_ref[e, 1], high) + dot(inv_ref[e, 0], low))


def pair_kernel(
    turn, arriving, early, where_ref, inv_ref, rhs_ref, mate_rhs_ref, own_ref, *rest,
):
    groups = min(HALF - turn, 3)
    foreign, rest = rest[: 3 * groups], rest[3 * groups :]
    seen, rest = rest[: len(arriving) + len(early)], rest[len(arriving) + len(early) :]
    acc_ref = None if turn else rest[0]
    prev_ref, out_ref = rest[-3:-1] if early else rest[-2:]
    sum_ref = rest[-1] if early else None
    pair, odd, half, parity = (where_ref[i] for i in range(4))

    def blocks(b):
        n, at = max(HALF - 1 - b, 0), 0
        if n >= 2:
            n, at = 2, b
        return own_ref[b], *(ref[at] for ref in foreign[3 * n : 3 * n + 3])

    def less(accs, b, x):
        own, other, mate, mate_other = blocks(b)
        mine, theirs = x[parity], x[1 - parity]
        return (
            accs[0] - (dot(own, mine) + dot(other, theirs)),
            accs[1] - (dot(mate, mine) + dot(mate_other, theirs)),
        )

    def fresh():
        return rhs_ref[:, pl.ds(pl.multiple_of(half * WIDE, WIDE), WIDE)], mate_rhs_ref[...]

    @pl.when(pair == turn)
    def _():
        accs = fresh() if turn else (acc_ref[0], acc_ref[1])
        for b, x in zip(arriving, seen):
            accs = less(accs, b, x)
        high = jnp.where(odd == 1, *accs)
        own, other, mate, mate_other = blocks(turn)
        between = jnp.where(
            odd == 0, jnp.where(parity == 1, own, other), jnp.where(parity == 1, mate, mate_other)
        )
        x_high = precise(inv_ref, 1, high).astype(jnp.bfloat16)
        low = jnp.where(odd == 0, *accs) - dot(between, x_high)
        out_ref[0] = precise(inv_ref, 0, low).astype(jnp.bfloat16)
        out_ref[1] = x_high

    @pl.when(pair != turn)
    def _():
        out_ref[...] = prev_ref[...]

    if early:
        @pl.when(pair == turn - 1)
        def _():
            accs = fresh()
            for b, x in zip(early, seen[len(arriving) :]):
                accs = less(accs, b, x)
            sum_ref[0], sum_ref[1] = accs


def final_kernel(
    where_ref, x_ref, w_own_ref, other3_ref, other2_ref, other01_ref, z_own_ref, z_other_ref,
    rhs_ref, pending_ref, image_ref,
):
    parity = where_ref[3]
    pending = rhs_ref[...]
    image = jnp.zeros_like(pending)
    for b in range(HALF):
        yl, xp = b // 2, b % 2
        own, other = w_own_ref[b], (other01_ref[b] if b < 2 else (other2_ref, other3_ref)[b - 2][0])
        for w, z, p in ((own, z_own_ref, parity), (other, z_other_ref, 1 - parity)):
            columns = []
            for half in range(2):
                at = [(((4 * p + i) * 2 + yl) * 2 + xp) * 2 + (half ^ xp) for i in range(4)]
                columns.append(jnp.concatenate([x_ref[n] for n in at], 0))
            x = jnp.concatenate(columns, 1)
            pending = pending - dot(w, x)
            image = image + dot(z[b], x)
    pending_ref[...] = pending
    image_ref[...] = image


def call(kernel, outs, scratch, *args, limit=12 << 20):
    vmem = pl.BlockSpec(memory_space=pltpu.VMEM)
    smem = pl.BlockSpec(memory_space=pltpu.SMEM)
    return pl.pallas_call(
        kernel,
        out_shape=outs,
        in_specs=[smem if a.dtype == jnp.int32 else vmem for a in args],
        out_specs=jax.tree.map(lambda _: vmem, outs),
        scratch_shapes=scratch,
        compiler_params=pltpu.CompilerParams(vmem_limit_bytes=limit),
    )(*args)


def to_pairs(a, moves):
    sends = []
    for src, dst in moves:
        for half in range(2):
            sends.append(tuple(2 * m + (half ^ (m % 2)) for m in (src, dst)))
    return lax.ppermute(a, ("yl", "xp", "xq"), sends)


def to_mate(a, full, partly):
    sends = []
    for m in full + partly:
        for odd, core in ((0, 1),) if m in partly else ((0, 0), (0, 1), (1, 0), (1, 1)):
            sends.append((4 * m + 2 * odd + core, 4 * m + 2 * (1 - odd) + core))
    return lax.ppermute(a, ("yl", "xp", "xq", "col"), sends)


def local(pencil_left, pencil_right, basis_panel, block_inverses, pencil_shift, start_vectors):
    row = lax.axis_index(ROWS)
    parity = lax.axis_index("col")
    pair = lax.axis_index(("yl", "xp"))
    odd = lax.axis_index("xq")
    half = odd ^ lax.axis_index("xp")
    where = jnp.stack([pair, odd, half, parity]).astype(jnp.int32)
    where, pencil_shift, lower_half = lax.optimization_barrier((where, pencil_shift, half == 0))
    first = lax.axis_size(ROWS) - STEPS

    left = pencil_left.reshape(NB, HALF, NB)
    right = pencil_right.reshape(NB, HALF, NB)
    own_z = jnp.transpose(basis_panel.reshape(NB, HALF, NB), (1, 0, 2))
    rhs = start_vectors.reshape(NB, NB)

    cols = 2 * jnp.arange(HALF) + parity
    live = (row < first + cols)[None, :, None]
    both = left.astype(jnp.float32) - pencil_shift * right.astype(jnp.float32)
    own = jnp.transpose(jnp.where(live, both, 0.0).astype(jnp.bfloat16), (1, 0, 2))
    own3 = own[HALF - 1 :]
    mate3 = to_mate(own3, [0, 1, 2], [3])
    other3 = lax.ppermute(own3, "col", FLIP)
    mate_rhs = lax.ppermute(jnp.where(lower_half, rhs[:, WIDE:], rhs[:, :WIDE]), "xq", FLIP)
    mate3_other = lax.ppermute(mate3, "col", FLIP)
    mate2 = to_mate(own[2:3], [0, 1], [2])
    other2 = lax.ppermute(own[2:3], "col", FLIP)
    inverses = call(
        split_kernel, jax.ShapeDtypeStruct((2, 2, NB, NB), jnp.bfloat16), [], where, block_inverses
    )
    mate01 = to_mate(own[:2], [0], [1])
    other01 = lax.ppermute(own[:2], "col", FLIP)
    mate2_other = lax.ppermute(mate2, "col", FLIP)
    mate01_other = lax.ppermute(mate01, "col", FLIP)
    other_z = lax.ppermute(own_z, "col", FLIP)

    shape = jax.ShapeDtypeStruct((2, NB, WIDE), jnp.bfloat16)
    sums = jax.ShapeDtypeStruct((2, NB, WIDE), jnp.float32)

    foreign = (
        (other3, mate3, mate3_other), (other2, mate2, mate2_other), (other01, mate01, mate01_other)
    )

    def solve(turn, arriving, early, *last):
        return call(
            functools.partial(pair_kernel, turn, [b for b, _ in arriving], [b for b, _ in early]),
            (shape, sums) if early else shape, [],
            where, inverses, rhs, mate_rhs, own, *sum(foreign[: HALF - turn], ()),
            *[x for _, x in arriving + early], *last,
        )

    x3 = solve(3, [], [], jnp.zeros(shape.shape, shape.dtype))
    a = to_pairs(x3, [(3, 2)])
    b = to_pairs(x3, [(3, 1)])
    x2 = solve(2, [(3, a)], [], x3)
    c = to_pairs(x2, [(2, 1), (3, 0)])
    d = to_pairs(x2, [(2, 0)])
    x1, acc = solve(1, [(3, b), (2, c)], [(3, c), (2, d)], x2)
    e = to_pairs(x1, [(1, 0)])
    x0 = solve(0, [(1, e)], [], acc, x1)

    spread = lax.all_to_all(
        x0.reshape(GROUPS, 2 * NB // GROUPS, WIDE), ("z", "yh"), 0, 0, tiled=True
    )[GROUPS - 1]
    spread, other_z = lax.optimization_barrier((spread, other_z))
    count = lax.axis_size(ROWS)
    every = lax.all_to_all(
        jnp.broadcast_to(spread[None], (count, *spread.shape)), ROWS, 0, 0, tiled=True
    )

    out = jax.ShapeDtypeStruct((NB, NB), jnp.float32)
    pending, image = call(
        final_kernel, (out, out), [],
        where, every, own, other3, other2, other01, own_z, other_z, rhs,
    )
    return pending.reshape(1, 1, NB, NB), image.reshape(1, 1, NB, NB)


def solution(mesh):
    fine = Mesh(mesh.devices.reshape(4, 2, 2, 2, 2, 2), (*ROWS, "col"))
    wide = P(None, ROWS, None, None, "col", None)
    tall = P(None, ROWS, None, "col")
    return jax.shard_map(
        local, mesh=fine, in_specs=(wide, wide, wide, P(), P(), tall),
        out_specs=(tall, tall), check_vma=False,
    )
```

```python
import functools

import jax
import jax.numpy as jnp
from jax import lax
from jax.experimental import pallas as pl
from jax.experimental.pallas import tpu as pltpu
from jax.sharding import Mesh, PartitionSpec as P


STEPS = 8
HALF = STEPS // 2
NB = 256
WIDE = NB // 2
DEPTH = 4
ROWS = ("z", "yh", "yl", "xp", "xq")
PLANE = ("z", "yl", "xp", "xq")
FLIP = [(0, 1), (1, 0)]


def dot(a, b):
    return jnp.dot(a, b, preferred_element_type=jnp.float32)


def halves(a):
    high = a.astype(jnp.bfloat16)
    return high, (a - high.astype(jnp.float32)).astype(jnp.bfloat16)


def split_kernel(where_ref, inv_ref, out_ref):
    for e in range(2):
        out_ref[e, 0], out_ref[e, 1] = halves(inv_ref[where_ref[0], e])


def precise(inv_ref, e, b):
    high, low = halves(b)
    return dot(inv_ref[e, 0], high) + (dot(inv_ref[e, 1], high) + dot(inv_ref[e, 0], low))


def pair_kernel(
    turn, arriving, early, where_ref, inv_ref, rhs_ref, mate_rhs_ref, own_ref, *rest,
):
    groups = min(HALF - turn, 3)
    foreign, rest = rest[: 3 * groups], rest[3 * groups :]
    seen, rest = rest[: len(arriving) + len(early)], rest[len(arriving) + len(early) :]
    acc_ref = None if turn else rest[0]
    prev_ref, out_ref = rest[-3:-1] if early else rest[-2:]
    sum_ref = rest[-1] if early else None
    pair, odd, half, parity = (where_ref[i] for i in range(4))

    def blocks(b):
        n, at = max(HALF - 1 - b, 0), 0
        if n >= 2:
            n, at = 2, b
        return own_ref[b], *(ref[at] for ref in foreign[3 * n : 3 * n + 3])

    def less(accs, b, x):
        own, other, mate, mate_other = blocks(b)
        mine, theirs = x[parity], x[1 - parity]
        return (
            accs[0] - (dot(own, mine) + dot(other, theirs)),
            accs[1] - (dot(mate, mine) + dot(mate_other, theirs)),
        )

    def fresh():
        return rhs_ref[:, pl.ds(pl.multiple_of(half * WIDE, WIDE), WIDE)], mate_rhs_ref[...]

    @pl.when(pair == turn)
    def _():
        accs = fresh() if turn else (acc_ref[0], acc_ref[1])
        for b, x in zip(arriving, seen):
            accs = less(accs, b, x)
        high = jnp.where(odd == 1, *accs)
        own, other, mate, mate_other = blocks(turn)
        between = jnp.where(
            odd == 0, jnp.where(parity == 1, own, other), jnp.where(parity == 1, mate, mate_other)
        )
        x_high = precise(inv_ref, 1, high).astype(jnp.bfloat16)
        low = jnp.where(odd == 0, *accs) - dot(between, x_high)
        out_ref[0] = precise(inv_ref, 0, low).astype(jnp.bfloat16)
        out_ref[1] = x_high

    @pl.when(pair != turn)
    def _():
        out_ref[...] = prev_ref[...]

    if early:
        @pl.when(pair == turn - 1)
        def _():
            accs = fresh()
            for b, x in zip(early, seen[len(arriving) :]):
                accs = less(accs, b, x)
            sum_ref[0], sum_ref[1] = accs


def pack_kernel(
    w_own_ref, other3_ref, other2_ref, other01_ref, z_own_ref, z_other_ref, out_ref
):
    for b in range(HALF):
        other = other01_ref[b] if b < 2 else (other2_ref, other3_ref)[b - 2][0]
        blocks = ((w_own_ref[b], other), (z_own_ref[b], z_other_ref[b]))
        for n in range(2):
            for side in range(2):
                at = (side * HALF + b) * NB
                out_ref[n, :, at : at + NB] = blocks[n][side]


def final_kernel(where_ref, x_ref, rows_ref, rhs_ref, pending_ref, image_ref, order_ref):
    parity = where_ref[3]
    for b in range(HALF):
        yl, xp = b // 2, b % 2
        for side, p in enumerate((parity, 1 - parity)):
            for half in range(2):
                for i in range(2):
                    at = (((2 * p + i) * 2 + yl) * 2 + xp) * 2 + (half ^ xp)
                    to = (side * HALF + b) * NB + i * WIDE
                    order_ref[to : to + WIDE, half * WIDE : (half + 1) * WIDE] = x_ref[at]
    x = order_ref[...]
    pending_ref[...] = rhs_ref[...] - dot(rows_ref[0], x)
    image_ref[...] = dot(rows_ref[1], x)


def call(kernel, outs, scratch, *args, limit=12 << 20):
    vmem = pl.BlockSpec(memory_space=pltpu.VMEM)
    smem = pl.BlockSpec(memory_space=pltpu.SMEM)
    return pl.pallas_call(
        kernel,
        out_shape=outs,
        in_specs=[smem if a.dtype == jnp.int32 else vmem for a in args],
        out_specs=jax.tree.map(lambda _: vmem, outs),
        scratch_shapes=scratch,
        compiler_params=pltpu.CompilerParams(vmem_limit_bytes=limit),
    )(*args)


def to_pairs(a, moves):
    sends = []
    for src, dst in moves:
        for half in range(2):
            sends.append(tuple(2 * m + (half ^ (m % 2)) for m in (src, dst)))
    return lax.ppermute(a, ("yl", "xp", "xq"), sends)


def local(pencil_left, pencil_right, basis_panel, block_inverses, pencil_shift, start_vectors):
    row = lax.axis_index(ROWS)
    parity = lax.axis_index("col")
    pair = lax.axis_index(("yl", "xp"))
    odd = lax.axis_index("xq")
    half = odd ^ lax.axis_index("xp")
    where = jnp.stack([pair, odd, half, parity]).astype(jnp.int32)
    where, pencil_shift, lower_half = lax.optimization_barrier((where, pencil_shift, half == 0))
    first = lax.axis_size(ROWS) - STEPS

    left = pencil_left.reshape(NB, HALF, NB)
    right = pencil_right.reshape(NB, HALF, NB)
    own_z = jnp.transpose(basis_panel.reshape(NB, HALF, NB), (1, 0, 2))
    rhs = start_vectors.reshape(NB, NB)

    cols = 2 * jnp.arange(HALF) + parity
    live = (row < first + cols)[None, :, None]
    both = left.astype(jnp.float32) - pencil_shift * right.astype(jnp.float32)
    own = jnp.transpose(jnp.where(live, both, 0.0).astype(jnp.bfloat16), (1, 0, 2))
    own3 = own[HALF - 1 :]
    mate3 = lax.ppermute(own3, "xq", FLIP)
    other3 = lax.ppermute(own3, "col", FLIP)
    mate_rhs = lax.ppermute(jnp.where(lower_half, rhs[:, WIDE:], rhs[:, :WIDE]), "xq", FLIP)
    mate3_other = lax.ppermute(mate3, "col", FLIP)
    mate2 = lax.ppermute(own[2:3], "xq", FLIP)
    other2 = lax.ppermute(own[2:3], "col", FLIP)
    inverses = call(
        split_kernel, jax.ShapeDtypeStruct((2, 2, NB, NB), jnp.bfloat16), [], where, block_inverses
    )
    mate01 = lax.ppermute(own[:2], "xq", FLIP)
    other01 = lax.ppermute(own[:2], "col", FLIP)
    mate2_other = lax.ppermute(mate2, "col", FLIP)
    mate01_other = lax.ppermute(mate01, "col", FLIP)
    other_z = lax.ppermute(own_z, "col", FLIP)

    shape = jax.ShapeDtypeStruct((2, NB, WIDE), jnp.bfloat16)
    sums = jax.ShapeDtypeStruct((2, NB, WIDE), jnp.float32)

    foreign = (
        (other3, mate3, mate3_other), (other2, mate2, mate2_other), (other01, mate01, mate01_other)
    )

    def solve(turn, arriving, early, *last):
        return call(
            functools.partial(pair_kernel, turn, [b for b, _ in arriving], [b for b, _ in early]),
            (shape, sums) if early else shape, [],
            where, inverses, rhs, mate_rhs, own, *sum(foreign[: HALF - turn], ()),
            *[x for _, x in arriving + early], *last,
        )

    x3 = solve(3, [], [], jnp.zeros(shape.shape, shape.dtype))
    a = to_pairs(x3, [(3, 2)])
    b = to_pairs(x3, [(3, 1)])
    x2 = solve(2, [(3, a)], [], x3)
    c = to_pairs(x2, [(2, 1), (3, 0)])
    d = to_pairs(x2, [(2, 0)])
    x1, acc = solve(1, [(3, b), (2, c)], [(3, c), (2, d)], x2)
    e = to_pairs(x1, [(1, 0)])
    rows = call(
        pack_kernel, jax.ShapeDtypeStruct((2, NB, STEPS * NB), jnp.bfloat16), [],
        own, other3, other2, other01, own_z, other_z,
    )
    x0 = solve(0, [(1, e)], [], acc, x1)

    quarters = x0.reshape(DEPTH, 1, 2 * NB // DEPTH, WIDE)
    quarters = jnp.broadcast_to(quarters, (DEPTH, 2, *quarters.shape[2:]))
    spread = lax.all_to_all(
        quarters.reshape(2 * DEPTH, *quarters.shape[2:]), ("z", "yh"), 0, 0, tiled=True
    )[2 * DEPTH - 1]
    spread, rows = lax.optimization_barrier((spread, rows))
    count = lax.axis_size(PLANE)
    every = lax.all_to_all(
        jnp.broadcast_to(spread[None], (count, *spread.shape)), PLANE, 0, 0, tiled=True
    )

    out = jax.ShapeDtypeStruct((NB, NB), jnp.float32)
    pending, image = call(
        final_kernel, (out, out), [pltpu.VMEM((STEPS * NB, NB), jnp.bfloat16)],
        where, every, rows, rhs,
    )
    return pending.reshape(1, 1, NB, NB), image.reshape(1, 1, NB, NB)


def solution(mesh):
    fine = Mesh(mesh.devices.reshape(4, 2, 2, 2, 2, 2), (*ROWS, "col"))
    wide = P(None, ROWS, None, None, "col", None)
    tall = P(None, ROWS, None, "col")
    return jax.shard_map(
        local, mesh=fine, in_specs=(wide, wide, wide, P(), P(), tall),
        out_specs=(tall, tall), check_vma=False,
    )
```

```python
import functools

import jax
import jax.numpy as jnp
from jax import lax
from jax.experimental import pallas as pl
from jax.experimental.pallas import tpu as pltpu
from jax.sharding import Mesh, PartitionSpec as P


STEPS = 8
HALF = STEPS // 2
NB = 256
WIDE = NB // 2
DEPTH = 4
ROWS = ("z", "yh", "yl", "xp", "xq")
PLANE = ("z", "yl", "xp", "xq")
FLIP = [(0, 1), (1, 0)]


def dot(a, b):
    return jnp.dot(a, b, preferred_element_type=jnp.float32)


def halves(a):
    high = a.astype(jnp.bfloat16)
    return high, (a - high.astype(jnp.float32)).astype(jnp.bfloat16)


def split_kernel(where_ref, inv_ref, out_ref):
    for e in range(2):
        out_ref[e, 0], out_ref[e, 1] = halves(inv_ref[where_ref[0], e])


def precise(inv_ref, e, b):
    high, low = halves(b)
    return dot(inv_ref[e, 0], high) + (dot(inv_ref[e, 1], high) + dot(inv_ref[e, 0], low))


def pair_kernel(
    turn, arriving, early, where_ref, inv_ref, rhs_ref, mate_rhs_ref, own_ref, *rest,
):
    groups = min(HALF - turn, 3)
    foreign, rest = rest[: 3 * groups], rest[3 * groups :]
    seen, rest = rest[: len(arriving) + len(early)], rest[len(arriving) + len(early) :]
    acc_ref = None if turn else rest[0]
    prev_ref, out_ref = rest[-3:-1] if early else rest[-2:]
    sum_ref = rest[-1] if early else None
    pair, odd, half, parity = (where_ref[i] for i in range(4))

    def blocks(b):
        n, at = max(HALF - 1 - b, 0), 0
        if n >= 2:
            n, at = 2, b
        return own_ref[b], *(ref[at] for ref in foreign[3 * n : 3 * n + 3])

    def less(accs, b, x):
        own, other, mate, mate_other = blocks(b)
        mine, theirs = x[parity], x[1 - parity]
        return (
            accs[0] - (dot(own, mine) + dot(other, theirs)),
            accs[1] - (dot(mate, mine) + dot(mate_other, theirs)),
        )

    def fresh():
        return rhs_ref[:, pl.ds(pl.multiple_of(half * WIDE, WIDE), WIDE)], mate_rhs_ref[...]

    @pl.when(pair == turn)
    def _():
        accs = fresh() if turn else (acc_ref[0], acc_ref[1])
        for b, x in zip(arriving, seen):
            accs = less(accs, b, x)
        high = jnp.where(odd == 1, *accs)
        own, other, mate, mate_other = blocks(turn)
        between = jnp.where(
            odd == 0, jnp.where(parity == 1, own, other), jnp.where(parity == 1, mate, mate_other)
        )
        x_high = precise(inv_ref, 1, high).astype(jnp.bfloat16)
        low = jnp.where(odd == 0, *accs) - dot(between, x_high)
        out_ref[0] = precise(inv_ref, 0, low).astype(jnp.bfloat16)
        out_ref[1] = x_high

    @pl.when(pair != turn)
    def _():
        out_ref[...] = prev_ref[...]

    if early:
        @pl.when(pair == turn - 1)
        def _():
            accs = fresh()
            for b, x in zip(early, seen[len(arriving) :]):
                accs = less(accs, b, x)
            sum_ref[0], sum_ref[1] = accs


def pack_kernel(
    w_own_ref, other3_ref, other2_ref, other01_ref, z_own_ref, z_other_ref, out_ref
):
    for b in range(HALF):
        other = other01_ref[b] if b < 2 else (other2_ref, other3_ref)[b - 2][0]
        blocks = ((w_own_ref[b], other), (z_own_ref[b], z_other_ref[b]))
        for n in range(2):
            for side in range(2):
                at = (side * HALF + b) * NB
                out_ref[n, :, at : at + NB] = blocks[n][side]


def final_kernel(
    where_ref, x_ref, rows_ref, rhs_ref, pending_out, image_out, order_ref, pending_ref, image_ref, sems
):
    parity = where_ref[3]
    for b in range(HALF):
        yl, xp = b // 2, b % 2
        for side, p in enumerate((parity, 1 - parity)):
            for half in range(2):
                for i in range(2):
                    at = (((2 * p + i) * 2 + yl) * 2 + xp) * 2 + (half ^ xp)
                    to = (side * HALF + b) * NB + i * WIDE
                    order_ref[to : to + WIDE, half * WIDE : (half + 1) * WIDE] = x_ref[at]
    x = order_ref[...]
    pending_ref[...] = rhs_ref[...] - dot(rows_ref[0], x)
    first = pltpu.make_async_copy(pending_ref, pending_out, sems.at[0])
    first.start()
    image_ref[...] = dot(rows_ref[1], x)
    second = pltpu.make_async_copy(image_ref, image_out, sems.at[1])
    second.start()
    first.wait()
    second.wait()


def call(kernel, outs, scratch, *args, limit=12 << 20, out_space=pltpu.VMEM):
    vmem = pl.BlockSpec(memory_space=pltpu.VMEM)
    smem = pl.BlockSpec(memory_space=pltpu.SMEM)
    result = pl.BlockSpec(memory_space=out_space)
    return pl.pallas_call(
        kernel,
        out_shape=outs,
        in_specs=[smem if a.dtype == jnp.int32 else vmem for a in args],
        out_specs=jax.tree.map(lambda _: result, outs),
        scratch_shapes=scratch,
        compiler_params=pltpu.CompilerParams(vmem_limit_bytes=limit),
    )(*args)


def to_pairs(a, moves):
    sends = []
    for src, dst in moves:
        for half in range(2):
            sends.append(tuple(2 * m + (half ^ (m % 2)) for m in (src, dst)))
    return lax.ppermute(a, ("yl", "xp", "xq"), sends)


def local(pencil_left, pencil_right, basis_panel, block_inverses, pencil_shift, start_vectors):
    row = lax.axis_index(ROWS)
    parity = lax.axis_index("col")
    pair = lax.axis_index(("yl", "xp"))
    odd = lax.axis_index("xq")
    half = odd ^ lax.axis_index("xp")
    where = jnp.stack([pair, odd, half, parity]).astype(jnp.int32)
    where, pencil_shift, lower_half = lax.optimization_barrier((where, pencil_shift, half == 0))
    first = lax.axis_size(ROWS) - STEPS

    left = pencil_left.reshape(NB, HALF, NB)
    right = pencil_right.reshape(NB, HALF, NB)
    own_z = jnp.transpose(basis_panel.reshape(NB, HALF, NB), (1, 0, 2))
    rhs = start_vectors.reshape(NB, NB)

    cols = 2 * jnp.arange(HALF) + parity
    live = (row < first + cols)[None, :, None]
    both = left.astype(jnp.float32) - pencil_shift * right.astype(jnp.float32)
    own = jnp.transpose(jnp.where(live, both, 0.0).astype(jnp.bfloat16), (1, 0, 2))
    own3 = own[HALF - 1 :]
    mate3 = lax.ppermute(own3, "xq", FLIP)
    other3 = lax.ppermute(own3, "col", FLIP)
    mate_rhs = lax.ppermute(jnp.where(lower_half, rhs[:, WIDE:], rhs[:, :WIDE]), "xq", FLIP)
    mate2 = lax.ppermute(own[2:3], "xq", FLIP)
    other2 = lax.ppermute(own[2:3], "col", FLIP)
    inverses = call(
        split_kernel, jax.ShapeDtypeStruct((2, 2, NB, NB), jnp.bfloat16), [], where, block_inverses
    )
    inverses, mate3 = lax.optimization_barrier((inverses, mate3))
    mate3_other = lax.ppermute(mate3, "col", FLIP)
    mate01 = lax.ppermute(own[:2], "xq", FLIP)
    other01 = lax.ppermute(own[:2], "col", FLIP)
    mate2_other = lax.ppermute(mate2, "col", FLIP)
    mate01_other = lax.ppermute(mate01, "col", FLIP)
    other_z = lax.ppermute(own_z, "col", FLIP)

    shape = jax.ShapeDtypeStruct((2, NB, WIDE), jnp.bfloat16)
    sums = jax.ShapeDtypeStruct((2, NB, WIDE), jnp.float32)

    foreign = (
        (other3, mate3, mate3_other), (other2, mate2, mate2_other), (other01, mate01, mate01_other)
    )

    def solve(turn, arriving, early, *last):
        return call(
            functools.partial(pair_kernel, turn, [b for b, _ in arriving], [b for b, _ in early]),
            (shape, sums) if early else shape, [],
            where, inverses, rhs, mate_rhs, own, *sum(foreign[: HALF - turn], ()),
            *[x for _, x in arriving + early], *last,
        )

    x3 = solve(3, [], [], jnp.zeros(shape.shape, shape.dtype))
    a = to_pairs(x3, [(3, 2)])
    b = to_pairs(x3, [(3, 1)])
    x2 = solve(2, [(3, a)], [], x3)
    c = to_pairs(x2, [(2, 1), (3, 0)])
    d = to_pairs(x2, [(2, 0)])
    x1, acc = solve(1, [(3, b), (2, c)], [(3, c), (2, d)], x2)
    e = to_pairs(x1, [(1, 0)])
    rows = call(
        pack_kernel, jax.ShapeDtypeStruct((2, NB, STEPS * NB), jnp.bfloat16), [],
        own, other3, other2, other01, own_z, other_z,
    )
    x0 = solve(0, [(1, e)], [], acc, x1)

    quarters = x0.reshape(DEPTH, 1, 2 * NB // DEPTH, WIDE)
    quarters = jnp.broadcast_to(quarters, (DEPTH, 2, *quarters.shape[2:]))
    spread = lax.all_to_all(
        quarters.reshape(2 * DEPTH, *quarters.shape[2:]), ("z", "yh"), 0, 0, tiled=True
    )[2 * DEPTH - 1]
    spread, rows = lax.optimization_barrier((spread, rows))
    count = lax.axis_size(PLANE)
    every = lax.all_to_all(
        jnp.broadcast_to(spread[None], (count, *spread.shape)), PLANE, 0, 0, tiled=True
    )

    out = jax.ShapeDtypeStruct((NB, NB), jnp.float32)
    pending, image = call(
        final_kernel, (out, out),
        [
            pltpu.VMEM((STEPS * NB, NB), jnp.bfloat16), pltpu.VMEM((NB, NB), jnp.float32),
            pltpu.VMEM((NB, NB), jnp.float32), pltpu.SemaphoreType.DMA((2,)),
        ],
        where, every, rows, rhs, out_space=pl.ANY,
    )
    return pending.reshape(1, 1, NB, NB), image.reshape(1, 1, NB, NB)


def solution(mesh):
    fine = Mesh(mesh.devices.reshape(4, 2, 2, 2, 2, 2), (*ROWS, "col"))
    wide = P(None, ROWS, None, None, "col", None)
    tall = P(None, ROWS, None, "col")
    return jax.shard_map(
        local, mesh=fine, in_specs=(wide, wide, wide, P(), P(), tall),
        out_specs=(tall, tall), check_vma=False,
    )
```

```python
import functools

import jax
import jax.numpy as jnp
from jax import lax
from jax.experimental import pallas as pl
from jax.experimental.pallas import tpu as pltpu
from jax.sharding import Mesh, PartitionSpec as P


STEPS = 8
HALF = STEPS // 2
NB = 256
WIDE = NB // 2
DEPTH = 4
ROWS = ("z", "yh", "yl", "xp", "xq")
PLANE = ("z", "yl", "xp", "xq")
FLIP = [(0, 1), (1, 0)]


def dot(a, b):
    return jnp.dot(a, b, preferred_element_type=jnp.float32)


def halves(a):
    high = a.astype(jnp.bfloat16)
    return high, (a - high.astype(jnp.float32)).astype(jnp.bfloat16)


def split_kernel(where_ref, inv_ref, out_ref):
    for e in range(2):
        out_ref[e, 0], out_ref[e, 1] = halves(inv_ref[where_ref[0], e])


def precise(inv_ref, e, b):
    high, low = halves(b)
    return dot(inv_ref[e, 0], high) + (dot(inv_ref[e, 1], high) + dot(inv_ref[e, 0], low))


def pair_kernel(
    turn, arriving, early, where_ref, inv_ref, rhs_ref, mate_rhs_ref, own_ref, *rest,
):
    groups = min(HALF - turn, 3)
    foreign, rest = rest[: 3 * groups], rest[3 * groups :]
    seen, rest = rest[: len(arriving) + len(early)], rest[len(arriving) + len(early) :]
    acc_ref = None if turn else rest[0]
    prev_ref, out_ref = rest[-3:-1] if early else rest[-2:]
    sum_ref = rest[-1] if early else None
    pair, odd, half, parity = (where_ref[i] for i in range(4))

    def blocks(b):
        n, at = max(HALF - 1 - b, 0), 0
        if n >= 2:
            n, at = 2, b
        return own_ref[b], *(ref[at] for ref in foreign[3 * n : 3 * n + 3])

    def less(accs, b, x):
        own, other, mate, mate_other = blocks(b)
        mine, theirs = x[parity], x[1 - parity]
        return (
            accs[0] - (dot(own, mine) + dot(other, theirs)),
            accs[1] - (dot(mate, mine) + dot(mate_other, theirs)),
        )

    def fresh():
        return rhs_ref[:, pl.ds(pl.multiple_of(half * WIDE, WIDE), WIDE)], mate_rhs_ref[...]

    @pl.when(pair == turn)
    def _():
        accs = fresh() if turn else (acc_ref[0], acc_ref[1])
        for b, x in zip(arriving, seen):
            accs = less(accs, b, x)
        high = jnp.where(odd == 1, *accs)
        own, other, mate, mate_other = blocks(turn)
        between = jnp.where(
            odd == 0, jnp.where(parity == 1, own, other), jnp.where(parity == 1, mate, mate_other)
        )
        x_high = precise(inv_ref, 1, high).astype(jnp.bfloat16)
        low = jnp.where(odd == 0, *accs) - dot(between, x_high)
        out_ref[0] = precise(inv_ref, 0, low).astype(jnp.bfloat16)
        out_ref[1] = x_high

    @pl.when(pair != turn)
    def _():
        out_ref[...] = prev_ref[...]

    if early:
        @pl.when(pair == turn - 1)
        def _():
            accs = fresh()
            for b, x in zip(early, seen[len(arriving) :]):
                accs = less(accs, b, x)
            sum_ref[0], sum_ref[1] = accs


def pack_kernel(
    w_own_ref, other3_ref, other2_ref, other01_ref, z_own_ref, z_other_ref, out_ref
):
    for b in range(HALF):
        other = other01_ref[b] if b < 2 else (other2_ref, other3_ref)[b - 2][0]
        blocks = ((w_own_ref[b], other), (z_own_ref[b], z_other_ref[b]))
        for n in range(2):
            for side in range(2):
                at = (side * HALF + b) * NB
                out_ref[n * NB : (n + 1) * NB, at : at + NB] = blocks[n][side]


def final_kernel(where_ref, x_ref, rows_ref, rhs_ref, pending_ref, image_ref, order_ref):
    parity = where_ref[3]
    for b in range(HALF):
        yl, xp = b // 2, b % 2
        for side, p in enumerate((parity, 1 - parity)):
            for half in range(2):
                for i in range(2):
                    at = (((2 * p + i) * 2 + yl) * 2 + xp) * 2 + (half ^ xp)
                    to = (side * HALF + b) * NB + i * WIDE
                    order_ref[to : to + WIDE, half * WIDE : (half + 1) * WIDE] = x_ref[at]
    x = order_ref[...]
    both = dot(rows_ref[...], x)
    pending_ref[...] = rhs_ref[...] - both[:NB]
    image_ref[...] = both[NB:]


def call(kernel, outs, scratch, *args, limit=12 << 20):
    vmem = pl.BlockSpec(memory_space=pltpu.VMEM)
    smem = pl.BlockSpec(memory_space=pltpu.SMEM)
    return pl.pallas_call(
        kernel,
        out_shape=outs,
        in_specs=[smem if a.dtype == jnp.int32 else vmem for a in args],
        out_specs=jax.tree.map(lambda _: vmem, outs),
        scratch_shapes=scratch,
        compiler_params=pltpu.CompilerParams(vmem_limit_bytes=limit),
    )(*args)


def to_pairs(a, moves):
    sends = []
    for src, dst in moves:
        for half in range(2):
            sends.append(tuple(2 * m + (half ^ (m % 2)) for m in (src, dst)))
    return lax.ppermute(a, ("yl", "xp", "xq"), sends)


def local(pencil_left, pencil_right, basis_panel, block_inverses, pencil_shift, start_vectors):
    row = lax.axis_index(ROWS)
    parity = lax.axis_index("col")
    pair = lax.axis_index(("yl", "xp"))
    odd = lax.axis_index("xq")
    half = odd ^ lax.axis_index("xp")
    where = jnp.stack([pair, odd, half, parity]).astype(jnp.int32)
    where, pencil_shift, lower_half = lax.optimization_barrier((where, pencil_shift, half == 0))
    first = lax.axis_size(ROWS) - STEPS

    left = pencil_left.reshape(NB, HALF, NB)
    right = pencil_right.reshape(NB, HALF, NB)
    own_z = jnp.transpose(basis_panel.reshape(NB, HALF, NB), (1, 0, 2))
    rhs = start_vectors.reshape(NB, NB)

    cols = 2 * jnp.arange(HALF) + parity
    live = (row < first + cols)[None, :, None]
    both = left.astype(jnp.float32) - pencil_shift * right.astype(jnp.float32)
    own = jnp.transpose(jnp.where(live, both, 0.0).astype(jnp.bfloat16), (1, 0, 2))
    own3 = own[HALF - 1 :]
    mate3 = lax.ppermute(own3, "xq", FLIP)
    other3 = lax.ppermute(own3, "col", FLIP)
    mate_rhs = lax.ppermute(jnp.where(lower_half, rhs[:, WIDE:], rhs[:, :WIDE]), "xq", FLIP)
    mate3_other = lax.ppermute(mate3, "col", FLIP)
    mate2 = lax.ppermute(own[2:3], "xq", FLIP)
    other2 = lax.ppermute(own[2:3], "col", FLIP)
    inverses = call(
        split_kernel, jax.ShapeDtypeStruct((2, 2, NB, NB), jnp.bfloat16), [], where, block_inverses
    )
    mate01 = lax.ppermute(own[:2], "xq", FLIP)
    other01 = lax.ppermute(own[:2], "col", FLIP)
    mate2_other = lax.ppermute(mate2, "col", FLIP)
    mate01_other = lax.ppermute(mate01, "col", FLIP)
    other_z = lax.ppermute(own_z, "col", FLIP)

    shape = jax.ShapeDtypeStruct((2, NB, WIDE), jnp.bfloat16)
    sums = jax.ShapeDtypeStruct((2, NB, WIDE), jnp.float32)

    foreign = (
        (other3, mate3, mate3_other), (other2, mate2, mate2_other), (other01, mate01, mate01_other)
    )

    def solve(turn, arriving, early, *last):
        return call(
            functools.partial(pair_kernel, turn, [b for b, _ in arriving], [b for b, _ in early]),
            (shape, sums) if early else shape, [],
            where, inverses, rhs, mate_rhs, own, *sum(foreign[: HALF - turn], ()),
            *[x for _, x in arriving + early], *last,
        )

    x3 = solve(3, [], [], jnp.zeros(shape.shape, shape.dtype))
    a = to_pairs(x3, [(3, 2)])
    b = to_pairs(x3, [(3, 1)])
    x2 = solve(2, [(3, a)], [], x3)
    c = to_pairs(x2, [(2, 1), (3, 0)])
    d = to_pairs(x2, [(2, 0)])
    x1, acc = solve(1, [(3, b), (2, c)], [(3, c), (2, d)], x2)
    e = to_pairs(x1, [(1, 0)])
    rows = call(
        pack_kernel, jax.ShapeDtypeStruct((2 * NB, STEPS * NB), jnp.bfloat16), [],
        own, other3, other2, other01, own_z, other_z,
    )
    x0 = solve(0, [(1, e)], [], acc, x1)

    quarters = x0.reshape(DEPTH, 1, 2 * NB // DEPTH, WIDE)
    quarters = jnp.broadcast_to(quarters, (DEPTH, 2, *quarters.shape[2:]))
    spread = lax.all_to_all(
        quarters.reshape(2 * DEPTH, *quarters.shape[2:]), ("z", "yh"), 0, 0, tiled=True
    )[2 * DEPTH - 1]
    spread, rows = lax.optimization_barrier((spread, rows))
    count = lax.axis_size(PLANE)
    every = lax.all_to_all(
        jnp.broadcast_to(spread[None], (count, *spread.shape)), PLANE, 0, 0, tiled=True
    )

    out = jax.ShapeDtypeStruct((NB, NB), jnp.float32)
    pending, image = call(
        final_kernel, (out, out), [pltpu.VMEM((STEPS * NB, NB), jnp.bfloat16)],
        where, every, rows, rhs,
    )
    return pending.reshape(1, 1, NB, NB), image.reshape(1, 1, NB, NB)


def solution(mesh):
    fine = Mesh(mesh.devices.reshape(4, 2, 2, 2, 2, 2), (*ROWS, "col"))
    wide = P(None, ROWS, None, None, "col", None)
    tall = P(None, ROWS, None, "col")
    return jax.shard_map(
        local, mesh=fine, in_specs=(wide, wide, wide, P(), P(), tall),
        out_specs=(tall, tall), check_vma=False,
    )
```

```python
import functools

import jax
import jax.numpy as jnp
from jax import lax
from jax.experimental import pallas as pl
from jax.experimental.pallas import tpu as pltpu
from jax.sharding import Mesh, PartitionSpec as P


STEPS = 8
HALF = STEPS // 2
NB = 256
WIDE = NB // 2
DEPTH = 4
ROWS = ("z", "yh", "yl", "xp", "xq")
PLANE = ("z", "yl", "xp", "xq")
FLIP = [(0, 1), (1, 0)]


def dot(a, b):
    return jnp.dot(a, b, preferred_element_type=jnp.float32)


def halves(a):
    high = a.astype(jnp.bfloat16)
    return high, (a - high.astype(jnp.float32)).astype(jnp.bfloat16)


def split_kernel(where_ref, inv_ref, out_ref):
    for e in range(2):
        out_ref[e, 0], out_ref[e, 1] = halves(inv_ref[where_ref[0], e])


def precise(inv_ref, e, b):
    high, low = halves(b)
    return dot(inv_ref[e, 0], high) + (dot(inv_ref[e, 1], high) + dot(inv_ref[e, 0], low))


def pair_kernel(
    turn, arriving, early, where_ref, inv_ref, rhs_ref, mate_rhs_ref, own_ref, *rest,
):
    groups = min(HALF - turn, 3)
    foreign, rest = rest[: 3 * groups], rest[3 * groups :]
    seen, rest = rest[: len(arriving) + len(early)], rest[len(arriving) + len(early) :]
    acc_ref = None if turn else rest[0]
    prev_ref, out_ref = rest[-3:-1] if early else rest[-2:]
    sum_ref = rest[-1] if early else None
    pair, odd, half, parity = (where_ref[i] for i in range(4))

    def blocks(b):
        n, at = max(HALF - 1 - b, 0), 0
        if n >= 2:
            n, at = 2, b
        return own_ref[b], *(ref[at] for ref in foreign[3 * n : 3 * n + 3])

    def less(accs, b, x):
        own, other, mate, mate_other = blocks(b)
        mine, theirs = x[parity], x[1 - parity]
        return (
            accs[0] - (dot(own, mine) + dot(other, theirs)),
            accs[1] - (dot(mate, mine) + dot(mate_other, theirs)),
        )

    def fresh():
        return rhs_ref[:, pl.ds(pl.multiple_of(half * WIDE, WIDE), WIDE)], mate_rhs_ref[...]

    @pl.when(pair == turn)
    def _():
        accs = fresh() if turn else (acc_ref[0], acc_ref[1])
        for b, x in zip(arriving, seen):
            accs = less(accs, b, x)
        high = jnp.where(odd == 1, *accs)
        own, other, mate, mate_other = blocks(turn)
        between = jnp.where(
            odd == 0, jnp.where(parity == 1, own, other), jnp.where(parity == 1, mate, mate_other)
        )
        x_high = precise(inv_ref, 1, high).astype(jnp.bfloat16)
        low = jnp.where(odd == 0, *accs) - dot(between, x_high)
        out_ref[0] = precise(inv_ref, 0, low).astype(jnp.bfloat16)
        out_ref[1] = x_high

    @pl.when(pair != turn)
    def _():
        out_ref[...] = prev_ref[...]

    if early:
        @pl.when(pair == turn - 1)
        def _():
            accs = fresh()
            for b, x in zip(early, seen[len(arriving) :]):
                accs = less(accs, b, x)
            sum_ref[0], sum_ref[1] = accs


def final_kernel(
    where_ref, x_ref, w_own_ref, other3_ref, other2_ref, other01_ref, z_own_ref, z_other_ref,
    rhs_ref, pending_ref, image_ref,
):
    parity = where_ref[3]
    pending = rhs_ref[...]
    image = jnp.zeros_like(pending)
    for b in range(HALF):
        yl, xp = b // 2, b % 2
        own, other = w_own_ref[b], (other01_ref[b] if b < 2 else (other2_ref, other3_ref)[b - 2][0])
        for w, z, p in ((own, z_own_ref, parity), (other, z_other_ref, 1 - parity)):
            columns = []
            for half in range(2):
                at = [(((2 * p + i) * 2 + yl) * 2 + xp) * 2 + (half ^ xp) for i in range(2)]
                columns.append(jnp.concatenate([x_ref[n] for n in at], 0))
            x = jnp.concatenate(columns, 1)
            pending = pending - dot(w, x)
            image = image + dot(z[b], x)
    pending_ref[...] = pending
    image_ref[...] = image


def call(kernel, outs, scratch, *args, limit=12 << 20):
    vmem = pl.BlockSpec(memory_space=pltpu.VMEM)
    smem = pl.BlockSpec(memory_space=pltpu.SMEM)
    return pl.pallas_call(
        kernel,
        out_shape=outs,
        in_specs=[smem if a.dtype == jnp.int32 else vmem for a in args],
        out_specs=jax.tree.map(lambda _: vmem, outs),
        scratch_shapes=scratch,
        compiler_params=pltpu.CompilerParams(vmem_limit_bytes=limit),
    )(*args)


def to_pairs(a, moves):
    sends = []
    for src, dst in moves:
        for half in range(2):
            sends.append(tuple(2 * m + (half ^ (m % 2)) for m in (src, dst)))
    return lax.ppermute(a, ("yl", "xp", "xq"), sends)


def local(pencil_left, pencil_right, basis_panel, block_inverses, pencil_shift, start_vectors):
    row = lax.axis_index(ROWS)
    parity = lax.axis_index("col")
    pair = lax.axis_index(("yl", "xp"))
    odd = lax.axis_index("xq")
    half = odd ^ lax.axis_index("xp")
    where = jnp.stack([pair, odd, half, parity]).astype(jnp.int32)
    where, pencil_shift, lower_half = lax.optimization_barrier((where, pencil_shift, half == 0))
    first = lax.axis_size(ROWS) - STEPS

    left = pencil_left.reshape(NB, HALF, NB)
    right = pencil_right.reshape(NB, HALF, NB)
    own_z = jnp.transpose(basis_panel.reshape(NB, HALF, NB), (1, 0, 2))
    rhs = start_vectors.reshape(NB, NB)

    cols = 2 * jnp.arange(HALF) + parity
    live = (row < first + cols)[None, :, None]
    both = left.astype(jnp.float32) - pencil_shift * right.astype(jnp.float32)
    own = jnp.transpose(jnp.where(live, both, 0.0).astype(jnp.bfloat16), (1, 0, 2))
    own3 = own[HALF - 1 :]
    mate3 = lax.ppermute(own3, "xq", FLIP)
    other3 = lax.ppermute(own3, "col", FLIP)
    mate_rhs = lax.ppermute(jnp.where(lower_half, rhs[:, WIDE:], rhs[:, :WIDE]), "xq", FLIP)
    mate3_other = lax.ppermute(mate3, "col", FLIP)
    mate2 = lax.ppermute(own[2:3], "xq", FLIP)
    other2 = lax.ppermute(own[2:3], "col", FLIP)
    inverses = call(
        split_kernel, jax.ShapeDtypeStruct((2, 2, NB, NB), jnp.bfloat16), [], where, block_inverses
    )
    mate01 = lax.ppermute(own[:2], "xq", FLIP)
    other01 = lax.ppermute(own[:2], "col", FLIP)
    mate2_other = lax.ppermute(mate2, "col", FLIP)
    mate01_other = lax.ppermute(mate01, "col", FLIP)
    other_z = lax.ppermute(own_z, "col", FLIP)

    shape = jax.ShapeDtypeStruct((2, NB, WIDE), jnp.bfloat16)
    sums = jax.ShapeDtypeStruct((2, NB, WIDE), jnp.float32)

    foreign = (
        (other3, mate3, mate3_other), (other2, mate2, mate2_other), (other01, mate01, mate01_other)
    )

    def solve(turn, arriving, early, *last):
        return call(
            functools.partial(pair_kernel, turn, [b for b, _ in arriving], [b for b, _ in early]),
            (shape, sums) if early else shape, [],
            where, inverses, rhs, mate_rhs, own, *sum(foreign[: HALF - turn], ()),
            *[x for _, x in arriving + early], *last,
        )

    x3 = solve(3, [], [], jnp.zeros(shape.shape, shape.dtype))
    a = to_pairs(x3, [(3, 2), (1, 3)])
    b = to_pairs(x3, [(3, 1)])
    x2 = solve(2, [(3, a)], [], x3)
    c = to_pairs(x2, [(2, 1), (3, 0), (0, 2), (1, 3)])
    d = to_pairs(x2, [(2, 0)])
    x1, acc = solve(1, [(3, b), (2, c)], [(3, c), (2, d)], x2)
    e = to_pairs(x1, [(1, 0), (3, 1)])
    x0 = solve(0, [(1, e)], [], acc, x1)

    quarters = x0.reshape(DEPTH, 1, 2 * NB // DEPTH, WIDE)
    quarters = jnp.broadcast_to(quarters, (DEPTH, 2, *quarters.shape[2:]))
    spread = lax.all_to_all(
        quarters.reshape(2 * DEPTH, *quarters.shape[2:]), ("z", "yh"), 0, 0, tiled=True
    )[2 * DEPTH - 1]
    spread, other_z = lax.optimization_barrier((spread, other_z))
    count = lax.axis_size(PLANE)
    every = lax.all_to_all(
        jnp.broadcast_to(spread[None], (count, *spread.shape)), PLANE, 0, 0, tiled=True
    )

    out = jax.ShapeDtypeStruct((NB, NB), jnp.float32)
    pending, image = call(
        final_kernel, (out, out), [],
        where, every, own, other3, other2, other01, own_z, other_z, rhs,
    )
    return pending.reshape(1, 1, NB, NB), image.reshape(1, 1, NB, NB)


def solution(mesh):
    fine = Mesh(mesh.devices.reshape(4, 2, 2, 2, 2, 2), (*ROWS, "col"))
    wide = P(None, ROWS, None, None, "col", None)
    tall = P(None, ROWS, None, "col")
    return jax.shard_map(
        local, mesh=fine, in_specs=(wide, wide, wide, P(), P(), tall),
        out_specs=(tall, tall), check_vma=False,
    )
```

```python
import functools

import jax
import jax.numpy as jnp
from jax import lax
from jax.experimental import pallas as pl
from jax.experimental.pallas import tpu as pltpu
from jax.sharding import Mesh, PartitionSpec as P


STEPS = 8
HALF = STEPS // 2
NB = 256
WIDE = NB // 2
DEPTH = 4
ROWS = ("z", "yh", "yl", "xp", "xq")
PLANE = ("yh", "yl", "xp", "xq")
FLIP = [(0, 1), (1, 0)]


def dot(a, b):
    return jnp.dot(a, b, preferred_element_type=jnp.float32)


def halves(a):
    high = a.astype(jnp.bfloat16)
    return high, (a - high.astype(jnp.float32)).astype(jnp.bfloat16)


def split_kernel(where_ref, inv_ref, out_ref):
    for e in range(2):
        out_ref[e, 0], out_ref[e, 1] = halves(inv_ref[where_ref[0], e])


def precise(inv_ref, e, b):
    high, low = halves(b)
    return dot(inv_ref[e, 0], high) + (dot(inv_ref[e, 1], high) + dot(inv_ref[e, 0], low))


def pair_kernel(
    turn, arriving, early, where_ref, inv_ref, rhs_ref, mate_rhs_ref, own_ref, *rest,
):
    groups = min(HALF - turn, 3)
    foreign, rest = rest[: 3 * groups], rest[3 * groups :]
    seen, rest = rest[: len(arriving) + len(early)], rest[len(arriving) + len(early) :]
    acc_ref = None if turn else rest[0]
    prev_ref, out_ref = rest[-3:-1] if early else rest[-2:]
    sum_ref = rest[-1] if early else None
    pair, odd, half, parity = (where_ref[i] for i in range(4))

    def blocks(b):
        n, at = max(HALF - 1 - b, 0), 0
        if n >= 2:
            n, at = 2, b
        return own_ref[b], *(ref[at] for ref in foreign[3 * n : 3 * n + 3])

    def less(accs, b, x):
        own, other, mate, mate_other = blocks(b)
        mine, theirs = x[parity], x[1 - parity]
        return (
            accs[0] - (dot(own, mine) + dot(other, theirs)),
            accs[1] - (dot(mate, mine) + dot(mate_other, theirs)),
        )

    def fresh():
        return rhs_ref[:, pl.ds(pl.multiple_of(half * WIDE, WIDE), WIDE)], mate_rhs_ref[...]

    @pl.when(pair == turn)
    def _():
        accs = fresh() if turn else (acc_ref[0], acc_ref[1])
        for b, x in zip(arriving, seen):
            accs = less(accs, b, x)
        high = jnp.where(odd == 1, *accs)
        own, other, mate, mate_other = blocks(turn)
        between = jnp.where(
            odd == 0, jnp.where(parity == 1, own, other), jnp.where(parity == 1, mate, mate_other)
        )
        x_high = precise(inv_ref, 1, high).astype(jnp.bfloat16)
        low = jnp.where(odd == 0, *accs) - dot(between, x_high)
        out_ref[0] = precise(inv_ref, 0, low).astype(jnp.bfloat16)
        out_ref[1] = x_high

    @pl.when(pair != turn)
    def _():
        out_ref[...] = prev_ref[...]

    if early:
        @pl.when(pair == turn - 1)
        def _():
            accs = fresh()
            for b, x in zip(early, seen[len(arriving) :]):
                accs = less(accs, b, x)
            sum_ref[0], sum_ref[1] = accs


def final_kernel(
    where_ref, x_ref, w_own_ref, other3_ref, other2_ref, other01_ref, z_own_ref, z_other_ref,
    rhs_ref, pending_ref, image_ref,
):
    parity = where_ref[3]
    pending = rhs_ref[...]
    image = jnp.zeros_like(pending)
    for b in range(HALF):
        yl, xp = b // 2, b % 2
        own, other = w_own_ref[b], (other01_ref[b] if b < 2 else (other2_ref, other3_ref)[b - 2][0])
        for w, z, p in ((own, z_own_ref, parity), (other, z_other_ref, 1 - parity)):
            x = jnp.concatenate([x_ref[((2 * p + yl) * 2 + xp) * 2 + (half ^ xp)] for half in range(2)], 1)
            pending = pending - dot(w, x)
            image = image + dot(z[b], x)
    pending_ref[...] = pending
    image_ref[...] = image


def call(kernel, outs, scratch, *args, limit=12 << 20):
    vmem = pl.BlockSpec(memory_space=pltpu.VMEM)
    smem = pl.BlockSpec(memory_space=pltpu.SMEM)
    return pl.pallas_call(
        kernel,
        out_shape=outs,
        in_specs=[smem if a.dtype == jnp.int32 else vmem for a in args],
        out_specs=jax.tree.map(lambda _: vmem, outs),
        scratch_shapes=scratch,
        compiler_params=pltpu.CompilerParams(vmem_limit_bytes=limit),
    )(*args)


def to_pairs(a, moves):
    sends = []
    for src, dst in moves:
        for half in range(2):
            sends.append(tuple(2 * m + (half ^ (m % 2)) for m in (src, dst)))
    return lax.ppermute(a, ("yl", "xp", "xq"), sends)


def local(pencil_left, pencil_right, basis_panel, block_inverses, pencil_shift, start_vectors):
    row = lax.axis_index(ROWS)
    parity = lax.axis_index("col")
    pair = lax.axis_index(("yl", "xp"))
    odd = lax.axis_index("xq")
    half = odd ^ lax.axis_index("xp")
    where = jnp.stack([pair, odd, half, parity]).astype(jnp.int32)
    where, pencil_shift, lower_half = lax.optimization_barrier((where, pencil_shift, half == 0))
    first = lax.axis_size(ROWS) - STEPS

    left = pencil_left.reshape(NB, HALF, NB)
    right = pencil_right.reshape(NB, HALF, NB)
    own_z = jnp.transpose(basis_panel.reshape(NB, HALF, NB), (1, 0, 2))
    rhs = start_vectors.reshape(NB, NB)

    cols = 2 * jnp.arange(HALF) + parity
    live = (row < first + cols)[None, :, None]
    both = left.astype(jnp.float32) - pencil_shift * right.astype(jnp.float32)
    own = jnp.transpose(jnp.where(live, both, 0.0).astype(jnp.bfloat16), (1, 0, 2))
    own3 = own[HALF - 1 :]
    mate3 = lax.ppermute(own3, "xq", FLIP)
    other3 = lax.ppermute(own3, "col", FLIP)
    mate_rhs = lax.ppermute(jnp.where(lower_half, rhs[:, WIDE:], rhs[:, :WIDE]), "xq", FLIP)
    mate3_other = lax.ppermute(mate3, "col", FLIP)
    mate2 = lax.ppermute(own[2:3], "xq", FLIP)
    other2 = lax.ppermute(own[2:3], "col", FLIP)
    inverses = call(
        split_kernel, jax.ShapeDtypeStruct((2, 2, NB, NB), jnp.bfloat16), [], where, block_inverses
    )
    mate01 = lax.ppermute(own[:2], "xq", FLIP)
    other01 = lax.ppermute(own[:2], "col", FLIP)
    mate2_other = lax.ppermute(mate2, "col", FLIP)
    mate01_other = lax.ppermute(mate01, "col", FLIP)
    other_z = lax.ppermute(own_z, "col", FLIP)

    shape = jax.ShapeDtypeStruct((2, NB, WIDE), jnp.bfloat16)
    sums = jax.ShapeDtypeStruct((2, NB, WIDE), jnp.float32)

    foreign = (
        (other3, mate3, mate3_other), (other2, mate2, mate2_other), (other01, mate01, mate01_other)
    )

    def solve(turn, arriving, early, *last):
        return call(
            functools.partial(pair_kernel, turn, [b for b, _ in arriving], [b for b, _ in early]),
            (shape, sums) if early else shape, [],
            where, inverses, rhs, mate_rhs, own, *sum(foreign[: HALF - turn], ()),
            *[x for _, x in arriving + early], *last,
        )

    x3 = solve(3, [], [], jnp.zeros(shape.shape, shape.dtype))
    a = to_pairs(x3, [(3, 2)])
    b = to_pairs(x3, [(3, 1)])
    x2 = solve(2, [(3, a)], [], x3)
    c = to_pairs(x2, [(2, 1), (3, 0)])
    d = to_pairs(x2, [(2, 0)])
    x1, acc = solve(1, [(3, b), (2, c)], [(3, c), (2, d)], x2)
    e = to_pairs(x1, [(1, 0)])
    x0 = solve(0, [(1, e)], [], acc, x1)

    spread = lax.all_to_all(
        jnp.broadcast_to(x0[None], (DEPTH, *x0.shape)).reshape(2 * DEPTH, *x0.shape[1:]),
        ("z", "yh"), 0, 0, tiled=True,
    )[2 * DEPTH - 1]
    spread, other_z = lax.optimization_barrier((spread, other_z))
    count = lax.axis_size(PLANE)
    every = lax.all_to_all(
        jnp.broadcast_to(spread[None], (count, *spread.shape)), PLANE, 0, 0, tiled=True
    )

    out = jax.ShapeDtypeStruct((NB, NB), jnp.float32)
    pending, image = call(
        final_kernel, (out, out), [],
        where, every, own, other3, other2, other01, own_z, other_z, rhs,
    )
    return pending.reshape(1, 1, NB, NB), image.reshape(1, 1, NB, NB)


def solution(mesh):
    fine = Mesh(mesh.devices.reshape(4, 2, 2, 2, 2, 2), (*ROWS, "col"))
    wide = P(None, ROWS, None, None, "col", None)
    tall = P(None, ROWS, None, "col")
    return jax.shard_map(
        local, mesh=fine, in_specs=(wide, wide, wide, P(), P(), tall),
        out_specs=(tall, tall), check_vma=False,
    )
```

```python
import functools

import jax
import jax.numpy as jnp
from jax import lax
from jax.experimental import pallas as pl
from jax.experimental.pallas import tpu as pltpu
from jax.sharding import Mesh, PartitionSpec as P


STEPS = 8
HALF = STEPS // 2
NB = 256
WIDE = NB // 2
DEPTH = 4
ROWS = ("z", "yh", "yl", "xp", "xq")
PLANE = ("z", "yl", "xp", "xq")
FLIP = [(0, 1), (1, 0)]


def dot(a, b):
    return jnp.dot(a, b, preferred_element_type=jnp.float32)


def halves(a):
    high = a.astype(jnp.bfloat16)
    return high, (a - high.astype(jnp.float32)).astype(jnp.bfloat16)


def split_kernel(where_ref, inv_ref, out_ref):
    for e in range(2):
        out_ref[e, 0], out_ref[e, 1] = halves(inv_ref[where_ref[0], e])


def precise(inv_ref, e, b):
    high, low = halves(b)
    both = dot(inv_ref[e].reshape(2 * NB, NB), high)
    return both[:NB] + (both[NB:] + dot(inv_ref[e, 0], low))


def pair_kernel(
    turn, arriving, early, where_ref, inv_ref, rhs_ref, mate_rhs_ref, own_ref, *rest,
):
    groups = min(HALF - turn, 3)
    foreign, rest = rest[: 3 * groups], rest[3 * groups :]
    seen, rest = rest[: len(arriving) + len(early)], rest[len(arriving) + len(early) :]
    acc_ref = None if turn else rest[0]
    prev_ref, out_ref = rest[-3:-1] if early else rest[-2:]
    sum_ref = rest[-1] if early else None
    pair, odd, half, parity = (where_ref[i] for i in range(4))

    def blocks(b):
        n, at = max(HALF - 1 - b, 0), 0
        if n >= 2:
            n, at = 2, b
        return own_ref[b], *(ref[at] for ref in foreign[3 * n : 3 * n + 3])

    def less(accs, b, x):
        own, other, mate, mate_other = blocks(b)
        mine, theirs = x[parity], x[1 - parity]
        step = dot(jnp.concatenate([own, mate], 0), mine) + dot(
            jnp.concatenate([other, mate_other], 0), theirs
        )
        return accs[0] - step[:NB], accs[1] - step[NB:]

    def fresh():
        return rhs_ref[:, pl.ds(pl.multiple_of(half * WIDE, WIDE), WIDE)], mate_rhs_ref[...]

    @pl.when(pair == turn)
    def _():
        accs = fresh() if turn else (acc_ref[0], acc_ref[1])
        for b, x in zip(arriving, seen):
            accs = less(accs, b, x)
        high = jnp.where(odd == 1, *accs)
        own, other, mate, mate_other = blocks(turn)
        between = jnp.where(
            odd == 0, jnp.where(parity == 1, own, other), jnp.where(parity == 1, mate, mate_other)
        )
        x_high = precise(inv_ref, 1, high).astype(jnp.bfloat16)
        low = jnp.where(odd == 0, *accs) - dot(between, x_high)
        out_ref[0] = precise(inv_ref, 0, low).astype(jnp.bfloat16)
        out_ref[1] = x_high

    @pl.when(pair != turn)
    def _():
        out_ref[...] = prev_ref[...]

    if early:
        @pl.when(pair == turn - 1)
        def _():
            accs = fresh()
            for b, x in zip(early, seen[len(arriving) :]):
                accs = less(accs, b, x)
            sum_ref[0], sum_ref[1] = accs


def final_kernel(
    where_ref, x_ref, w_own_ref, other3_ref, other2_ref, other01_ref, z_own_ref, z_other_ref,
    rhs_ref, pending_ref, image_ref,
):
    parity = where_ref[3]
    pending = rhs_ref[...]
    image = jnp.zeros_like(pending)
    for b in range(HALF):
        yl, xp = b // 2, b % 2
        own, other = w_own_ref[b], (other01_ref[b] if b < 2 else (other2_ref, other3_ref)[b - 2][0])
        for w, z, p in ((own, z_own_ref, parity), (other, z_other_ref, 1 - parity)):
            columns = []
            for half in range(2):
                at = [(((2 * p + i) * 2 + yl) * 2 + xp) * 2 + (half ^ xp) for i in range(2)]
                columns.append(jnp.concatenate([x_ref[n] for n in at], 0))
            x = jnp.concatenate(columns, 1)
            pending = pending - dot(w, x)
            image = image + dot(z[b], x)
    pending_ref[...] = pending
    image_ref[...] = image


def call(kernel, outs, scratch, *args, limit=12 << 20):
    vmem = pl.BlockSpec(memory_space=pltpu.VMEM)
    smem = pl.BlockSpec(memory_space=pltpu.SMEM)
    return pl.pallas_call(
        kernel,
        out_shape=outs,
        in_specs=[smem if a.dtype == jnp.int32 else vmem for a in args],
        out_specs=jax.tree.map(lambda _: vmem, outs),
        scratch_shapes=scratch,
        compiler_params=pltpu.CompilerParams(vmem_limit_bytes=limit),
    )(*args)


def to_pairs(a, moves):
    sends = []
    for src, dst in moves:
        for half in range(2):
            sends.append(tuple(2 * m + (half ^ (m % 2)) for m in (src, dst)))
    return lax.ppermute(a, ("yl", "xp", "xq"), sends)


def local(pencil_left, pencil_right, basis_panel, block_inverses, pencil_shift, start_vectors):
    row = lax.axis_index(ROWS)
    parity = lax.axis_index("col")
    pair = lax.axis_index(("yl", "xp"))
    odd = lax.axis_index("xq")
    half = odd ^ lax.axis_index("xp")
    where = jnp.stack([pair, odd, half, parity]).astype(jnp.int32)
    where, pencil_shift, lower_half = lax.optimization_barrier((where, pencil_shift, half == 0))
    first = lax.axis_size(ROWS) - STEPS

    left = pencil_left.reshape(NB, HALF, NB)
    right = pencil_right.reshape(NB, HALF, NB)
    own_z = jnp.transpose(basis_panel.reshape(NB, HALF, NB), (1, 0, 2))
    rhs = start_vectors.reshape(NB, NB)

    cols = 2 * jnp.arange(HALF) + parity
    live = (row < first + cols)[None, :, None]
    both = left.astype(jnp.float32) - pencil_shift * right.astype(jnp.float32)
    own = jnp.transpose(jnp.where(live, both, 0.0).astype(jnp.bfloat16), (1, 0, 2))
    own3 = own[HALF - 1 :]
    mate3 = lax.ppermute(own3, "xq", FLIP)
    other3 = lax.ppermute(own3, "col", FLIP)
    mate_rhs = lax.ppermute(jnp.where(lower_half, rhs[:, WIDE:], rhs[:, :WIDE]), "xq", FLIP)
    mate3_other = lax.ppermute(mate3, "col", FLIP)
    mate2 = lax.ppermute(own[2:3], "xq", FLIP)
    other2 = lax.ppermute(own[2:3], "col", FLIP)
    inverses = call(
        split_kernel, jax.ShapeDtypeStruct((2, 2, NB, NB), jnp.bfloat16), [], where, block_inverses
    )
    mate01 = lax.ppermute(own[:2], "xq", FLIP)
    other01 = lax.ppermute(own[:2], "col", FLIP)
    mate2_other = lax.ppermute(mate2, "col", FLIP)
    mate01_other = lax.ppermute(mate01, "col", FLIP)
    other_z = lax.ppermute(own_z, "col", FLIP)

    shape = jax.ShapeDtypeStruct((2, NB, WIDE), jnp.bfloat16)
    sums = jax.ShapeDtypeStruct((2, NB, WIDE), jnp.float32)

    foreign = (
        (other3, mate3, mate3_other), (other2, mate2, mate2_other), (other01, mate01, mate01_other)
    )

    def solve(turn, arriving, early, *last):
        return call(
            functools.partial(pair_kernel, turn, [b for b, _ in arriving], [b for b, _ in early]),
            (shape, sums) if early else shape, [],
            where, inverses, rhs, mate_rhs, own, *sum(foreign[: HALF - turn], ()),
            *[x for _, x in arriving + early], *last,
        )

    x3 = solve(3, [], [], jnp.zeros(shape.shape, shape.dtype))
    a = to_pairs(x3, [(3, 2)])
    b = to_pairs(x3, [(3, 1)])
    x2 = solve(2, [(3, a)], [], x3)
    c = to_pairs(x2, [(2, 1), (3, 0)])
    d = to_pairs(x2, [(2, 0)])
    x1, acc = solve(1, [(3, b), (2, c)], [(3, c), (2, d)], x2)
    e = to_pairs(x1, [(1, 0)])
    x0 = solve(0, [(1, e)], [], acc, x1)

    quarters = x0.reshape(DEPTH, 1, 2 * NB // DEPTH, WIDE)
    quarters = jnp.broadcast_to(quarters, (DEPTH, 2, *quarters.shape[2:]))
    spread = lax.all_to_all(
        quarters.reshape(2 * DEPTH, *quarters.shape[2:]), ("z", "yh"), 0, 0, tiled=True
    )[2 * DEPTH - 1]
    spread, other_z = lax.optimization_barrier((spread, other_z))
    count = lax.axis_size(PLANE)
    every = lax.all_to_all(
        jnp.broadcast_to(spread[None], (count, *spread.shape)), PLANE, 0, 0, tiled=True
    )

    out = jax.ShapeDtypeStruct((NB, NB), jnp.float32)
    pending, image = call(
        final_kernel, (out, out), [],
        where, every, own, other3, other2, other01, own_z, other_z, rhs,
    )
    return pending.reshape(1, 1, NB, NB), image.reshape(1, 1, NB, NB)


def solution(mesh):
    fine = Mesh(mesh.devices.reshape(4, 2, 2, 2, 2, 2), (*ROWS, "col"))
    wide = P(None, ROWS, None, None, "col", None)
    tall = P(None, ROWS, None, "col")
    return jax.shard_map(
        local, mesh=fine, in_specs=(wide, wide, wide, P(), P(), tall),
        out_specs=(tall, tall), check_vma=False,
    )
```

```python
import functools

import jax
import jax.numpy as jnp
from jax import lax
from jax.experimental import pallas as pl
from jax.experimental.pallas import tpu as pltpu
from jax.sharding import Mesh, PartitionSpec as P


STEPS = 8
HALF = STEPS // 2
NB = 256
WIDE = NB // 2
DEPTH = 4
ROWS = ("z", "yh", "yl", "xp", "xq")
PLANE = ("z", "yl", "xp", "xq")
FLIP = [(0, 1), (1, 0)]


def dot(a, b):
    return jnp.dot(a, b, preferred_element_type=jnp.float32)


def halves(a):
    high = a.astype(jnp.bfloat16)
    return high, (a - high.astype(jnp.float32)).astype(jnp.bfloat16)


def split_kernel(where_ref, inv_ref, out_ref):
    for e in range(2):
        out_ref[e, 0], out_ref[e, 1] = halves(inv_ref[where_ref[0], e])


def precise(inv_ref, e, b):
    high, low = halves(b)
    return dot(inv_ref[e, 0], high) + (dot(inv_ref[e, 1], high) + dot(inv_ref[e, 0], low))


def pair_kernel(
    turn, arriving, early, where_ref, inv_ref, rhs_ref, mate_rhs_ref, own_ref, *rest,
):
    groups = min(HALF - turn, 3)
    foreign, rest = rest[: 3 * groups], rest[3 * groups :]
    seen, rest = rest[: len(arriving) + len(early)], rest[len(arriving) + len(early) :]
    acc_ref = None if turn else rest[0]
    prev_ref, out_ref = rest[-3:-1] if early else rest[-2:]
    sum_ref = rest[-1] if early else None
    pair, odd, half, parity = (where_ref[i] for i in range(4))

    def blocks(b):
        n, at = max(HALF - 1 - b, 0), 0
        if n >= 2:
            n, at = 2, b
        return own_ref[b], *(ref[at] for ref in foreign[3 * n : 3 * n + 3])

    def less(accs, b, x):
        own, other, mate, mate_other = blocks(b)
        mine, theirs = x[parity], x[1 - parity]
        return (
            accs[0] - (dot(own, mine) + dot(other, theirs)),
            accs[1] - (dot(mate, mine) + dot(mate_other, theirs)),
        )

    def fresh():
        return rhs_ref[:, pl.ds(pl.multiple_of(half * WIDE, WIDE), WIDE)], mate_rhs_ref[...]

    @pl.when(pair == turn)
    def _():
        accs = fresh() if turn else (acc_ref[0], acc_ref[1])
        for b, x in zip(arriving, seen):
            accs = less(accs, b, x)
        high = jnp.where(odd == 1, *accs)
        own, other, mate, mate_other = blocks(turn)
        between = jnp.where(
            odd == 0, jnp.where(parity == 1, own, other), jnp.where(parity == 1, mate, mate_other)
        )
        x_high = precise(inv_ref, 1, high).astype(jnp.bfloat16)
        low = jnp.where(odd == 0, *accs) - dot(between, x_high)
        out_ref[0] = precise(inv_ref, 0, low).astype(jnp.bfloat16)
        out_ref[1] = x_high

    @pl.when(pair != turn)
    def _():
        out_ref[...] = prev_ref[...]

    if early:
        @pl.when(pair == turn - 1)
        def _():
            accs = fresh()
            for b, x in zip(early, seen[len(arriving) :]):
                accs = less(accs, b, x)
            sum_ref[0], sum_ref[1] = accs


def final_kernel(
    where_ref, x_ref, w_own_ref, other3_ref, other2_ref, other01_ref, z_own_ref, z_other_ref,
    rhs_ref, pending_ref, image_ref,
):
    parity = where_ref[3]
    pending = rhs_ref[...]
    image = jnp.zeros_like(pending)
    for b in range(HALF):
        yl, xp = b // 2, b % 2
        own, other = w_own_ref[b], (other01_ref[b] if b < 2 else (other2_ref, other3_ref)[b - 2][0])
        for w, z, p in ((own, z_own_ref, parity), (other, z_other_ref, 1 - parity)):
            columns = []
            for half in range(2):
                at = [(((2 * p + i) * 2 + yl) * 2 + xp) * 2 + (half ^ xp) for i in range(2)]
                columns.append(jnp.concatenate([x_ref[n] for n in at], 0))
            x = jnp.concatenate(columns, 1)
            pending = pending - dot(w, x)
            image = image + dot(z[b], x)
    pending_ref[...] = pending
    image_ref[...] = image


def call(kernel, outs, scratch, *args, limit=12 << 20):
    vmem = pl.BlockSpec(memory_space=pltpu.VMEM)
    smem = pl.BlockSpec(memory_space=pltpu.SMEM)
    return pl.pallas_call(
        kernel,
        out_shape=outs,
        in_specs=[smem if a.dtype == jnp.int32 else vmem for a in args],
        out_specs=jax.tree.map(lambda _: vmem, outs),
        scratch_shapes=scratch,
        compiler_params=pltpu.CompilerParams(vmem_limit_bytes=limit),
    )(*args)


def to_pairs(a, moves):
    sends = []
    for src, dst in moves:
        for half in range(2):
            sends.append(tuple(2 * m + (half ^ (m % 2)) for m in (src, dst)))
    return lax.ppermute(a, ("yl", "xp", "xq"), sends)


def local(pencil_left, pencil_right, basis_panel, block_inverses, pencil_shift, start_vectors):
    row = lax.axis_index(ROWS)
    parity = lax.axis_index("col")
    pair = lax.axis_index(("yl", "xp"))
    odd = lax.axis_index("xq")
    half = odd ^ lax.axis_index("xp")
    where = jnp.stack([pair, odd, half, parity]).astype(jnp.int32)
    where, pencil_shift, lower_half = lax.optimization_barrier((where, pencil_shift, half == 0))
    first = lax.axis_size(ROWS) - STEPS

    left = pencil_left.reshape(NB, HALF, NB)
    right = pencil_right.reshape(NB, HALF, NB)
    own_z = jnp.transpose(basis_panel.reshape(NB, HALF, NB), (1, 0, 2))
    rhs = start_vectors.reshape(NB, NB)

    cols = 2 * jnp.arange(HALF) + parity
    live = (row < first + cols)[None, :, None]
    both = left.astype(jnp.float32) - pencil_shift * right.astype(jnp.float32)
    own = jnp.transpose(jnp.where(live, both, 0.0).astype(jnp.bfloat16), (1, 0, 2))
    own3 = own[HALF - 1 :]
    mate3 = lax.ppermute(own3, "xq", FLIP)
    other3 = lax.ppermute(own3, "col", FLIP)
    mate_rhs = lax.ppermute(jnp.where(lower_half, rhs[:, WIDE:], rhs[:, :WIDE]), "xq", FLIP)
    mate3_other = lax.ppermute(mate3, "col", FLIP)
    mate2 = lax.ppermute(own[2:3], "xq", FLIP)
    other2 = lax.ppermute(own[2:3], "col", FLIP)
    inverses = call(
        split_kernel, jax.ShapeDtypeStruct((2, 2, NB, NB), jnp.bfloat16), [], where, block_inverses
    )
    mate01 = lax.ppermute(own[:2], "xq", FLIP)
    other01 = lax.ppermute(own[:2], "col", FLIP)
    mate2_other = lax.ppermute(mate2, "col", FLIP)
    mate01_other = lax.ppermute(mate01, "col", FLIP)
    other_z = lax.ppermute(own_z, "col", FLIP)

    shape = jax.ShapeDtypeStruct((2, NB, WIDE), jnp.bfloat16)
    sums = jax.ShapeDtypeStruct((2, NB, WIDE), jnp.float32)

    foreign = (
        (other3, mate3, mate3_other), (other2, mate2, mate2_other), (other01, mate01, mate01_other)
    )

    def solve(turn, arriving, early, *last):
        return call(
            functools.partial(pair_kernel, turn, [b for b, _ in arriving], [b for b, _ in early]),
            (shape, sums) if early else shape, [],
            where, inverses, rhs, mate_rhs, own, *sum(foreign[: HALF - turn], ()),
            *[x for _, x in arriving + early], *last,
        )

    x3 = solve(3, [], [], jnp.zeros(shape.shape, shape.dtype))
    a = to_pairs(x3, [(3, 2)])
    b = to_pairs(x3, [(3, 1)])
    x2 = solve(2, [(3, a)], [], x3)
    c = to_pairs(x2, [(2, 1), (3, 0)])
    d = to_pairs(x2, [(2, 0)])
    x1, acc = solve(1, [(3, b), (2, c)], [(3, c), (2, d)], x2)
    e = to_pairs(x1, [(1, 0)])
    x0 = solve(0, [(1, e)], [], acc, x1)

    quarters = x0.reshape(DEPTH, 1, 2 * NB // DEPTH, WIDE)
    quarters = jnp.broadcast_to(quarters, (DEPTH, 2, *quarters.shape[2:]))
    spread = lax.all_to_all(
        quarters.reshape(2 * DEPTH, *quarters.shape[2:]), ("z", "yh"), 0, 0, tiled=True
    )[2 * DEPTH - 1]
    spread, other_z = lax.optimization_barrier((spread, other_z))
    count = lax.axis_size(PLANE)
    every = lax.all_to_all(
        jnp.broadcast_to(spread[None], (count, *spread.shape)), PLANE, 0, 0, tiled=True
    )

    out = jax.ShapeDtypeStruct((NB, NB), jnp.float32)
    pending, image = call(
        final_kernel, (out, out), [],
        where, every, own, other3, other2, other01, own_z, other_z, rhs,
    )
    return pending.reshape(1, 1, NB, NB), image.reshape(1, 1, NB, NB)


def solution(mesh):
    fine = Mesh(mesh.devices.reshape(4, 2, 2, 2, 2, 2), (*ROWS, "col"))
    wide = P(None, ROWS, None, None, "col", None)
    tall = P(None, ROWS, None, "col")
    return jax.shard_map(
        local, mesh=fine, in_specs=(wide, wide, wide, P(), P(), tall),
        out_specs=(tall, tall), check_vma=False,
    )
```
